32 devices in a mesh: grp: 2 (over x), ctx: 16 (over z, y, core).
Axes of the slice: x: 2, y: 2, z: 4, core: 2. Of those that a mesh axis runs over, the one named last changes fastest.
Arguments:
- queries: bfloat16 [2, 24, 64, 576], P('grp', None, 'ctx'), parts along dimension 0, may hold values from -40 to 40
- cache: bfloat16 [2, 8192, 576], P('grp', 'ctx'), parts along dimension 0, may hold values from -6 to 6
- draft_latent: bfloat16 [2, 24, 576], P('grp'), parts along dimension 0, may hold values from -9 to 9
- lengths: int32 [2], P('grp'), parts along dimension 0, may hold values from 4096 to 8192
- parents: int32 [2, 24], P('grp'), parts along dimension 0, may hold values from -1 to 22, as said below
- value_up: bfloat16 [64, 512, 128], P('ctx'), may hold values from -0.25 to 0.25
- out_proj: bfloat16 [8192, 7168], P('ctx'), may hold values from -0.09375 to 0.09375
Outputs:
- attended: bfloat16 [48, 7168], P('grp', 'ctx'), parts along dimension 0
The draws below stay inside these ranges and needn't reach their ends.
There are 2 independent parts, one for each index of `grp`. The reference program is written for one: setup_inputs(seed, part) draws one part's arguments, and reference() takes and returns one part's arrays. A program takes and returns all parts, laid end to end along the dimension named above; an argument that names none is the same for every part. Nothing has to cross between parts.
Inputs may be any that keep to these rules, and one draw needn't show every extreme that they name: parents[r, 0] = -1 and 0 <= parents[r, i] < i for i >= 1.
All inputs are finite; a program needn't handle non-finite values.
Results may differ from the reference program's by a relative error of at most 0.007.
Values may be sent and summed in bfloat16 or wider, within the bound.
No kernel may reach another device: no remote copies, remote signals or barrier semaphores. Data moves between devices by JAX's collectives and lax.ppermute only.
A program may use at most 64 MiB of HBM per device.

```python
import math
import jax
import jax.numpy as jnp
from jax import lax

HEADS = 64
LATENT = 512
ROPE_DIM = 64
VALUE_DIM = 128
MODEL = 7168
DRAFT = 24
REQS = 1
CTX_DEV = 512
CTX = 8192
N_CTX = 16


def latent_pack(key):
    base = jax.random.fold_in(key, 71)
    width = LATENT + ROPE_DIM
    noise = jax.random.normal(jax.random.fold_in(base, 1), (REQS, CTX, width), jnp.float32)
    values = jnp.clip(noise, -6.0, 6.0)
    return values


def draw_cache(key, part):
    values = latent_pack(key)
    return values.astype(jnp.bfloat16)


def draw_queries(key, part):
    shape = (REQS, DRAFT, HEADS, LATENT + ROPE_DIM)
    values = jnp.clip(0.83 * jax.random.normal(jax.random.fold_in(key, 81), shape, jnp.float32), -5.0, 5.0)
    return values.astype(jnp.bfloat16)


def draw_parents(key, part):
    picks = jax.random.randint(jax.random.fold_in(key, 91), (REQS, DRAFT), 0, 1 << 20)
    order = jnp.arange(DRAFT, dtype=jnp.int32)[None, :]
    chosen = picks % jnp.maximum(order, 1)
    return jnp.where(order == 0, -1, chosen).astype(jnp.int32)


def strengthened(values, own_key, source, target, blocks, factor):
    def block_of(position):
        return (jnp.arange(values.shape[position]) // (values.shape[position] // blocks)).reshape((-1,) + (1,) * (values.ndim - 1 - position))

    one_side = jax.random.permutation(own_key, blocks)[block_of(target)]
    second = (block_of(target) + blocks // 2) % blocks
    return jnp.where((block_of(source) == one_side) | (block_of(source) == second), factor * values, values)


def steps_of(own_key, dims, cuts, smallest, largest):
    def one(axis_at, blocks):
        steps = jax.random.uniform(jax.random.fold_in(jax.random.fold_in(own_key, 6), axis_at), (blocks,), jnp.float32, smallest / len(cuts), largest / len(cuts))
        return jnp.repeat(jnp.exp(steps), dims[axis_at] // blocks).reshape((-1,) + (1,) * (len(dims) - axis_at - 1))

    level = one(*cuts[0])
    for cut in cuts[1:]:
        level = level * one(*cut)
    return level


def normal_values(key, shape, scale, most, split=(), kind=jnp.bfloat16):
    factor_of = steps_of(key, shape, split, -0.22, 0.18) if split else 1.0
    values = jax.random.normal(key, shape, jnp.float32) * scale * factor_of
    return jnp.minimum(jnp.maximum(values, -most), most).astype(kind)


def heavy_noise(key, shape, spread, most, split, heavy, kind=jnp.bfloat16):
    entries = spread * jax.random.normal(key, shape, jnp.float32)
    if split:
        entries = entries * steps_of(key, shape, split, -0.22, 0.18)
    return jnp.clip(strengthened(entries, jax.random.fold_in(key, 3), *heavy), -most, most).astype(kind)


def setup_inputs(seed: int = 0, part: int = 0) -> dict:
    key_of = jax.random.split(jax.random.key(seed), 8)
    own_keys = jax.random.split(jax.random.fold_in(key_of[7], part), 8)
    return {
        "queries": draw_queries(jax.random.fold_in(jax.random.fold_in(key_of[7], part), 71), part),
        "cache": draw_cache(jax.random.fold_in(jax.random.fold_in(key_of[7], part), 71), part),
        "draft_latent": normal_values(own_keys[2], (REQS, DRAFT, LATENT + ROPE_DIM), 1.5, 9.0),
        "lengths": jax.random.randint(own_keys[3], (REQS,), CTX // 2, CTX + 1).astype(jnp.int32),
        "parents": draw_parents(jax.random.fold_in(jax.random.fold_in(key_of[7], part), 71), part),
        "value_up": normal_values(key_of[5], (HEADS, LATENT, VALUE_DIM), LATENT ** -0.5, 0.25, ((0, 16),)),
        "out_proj": heavy_noise(key_of[6], (HEADS * VALUE_DIM, MODEL), (HEADS * VALUE_DIM) ** -0.5, 0.09375, ((0, 16),), (0, 1, 16, 2.0)),
    }


yarn_factor = 1.0 + 0.1 * math.log(32.0)
score_scale = yarn_factor * yarn_factor / math.sqrt(192.0)
neg_fill = -1e+30

def tree_reach(parents):
    drafts = parents.shape[1]
    order = jnp.arange(drafts, dtype=jnp.int32)
    adjacent = (parents[:, :, None] == order[None, None, :]).astype(jnp.float32)
    ident = jnp.broadcast_to(jnp.eye(drafts, dtype=jnp.float32), adjacent.shape)

    def extend(step, reach):
        grown = ident + jnp.einsum('rij,rjk->rik', adjacent, reach, precision=lax.Precision.HIGHEST)
        return jnp.minimum(grown, 1.0)
    return lax.fori_loop(0, drafts, extend, ident) > 0.5

def single_state(rows, keys, valid):
    scores = lax.dot_general(rows, keys, (((1,), (1,)), ((), ())), preferred_element_type=jnp.float32) * score_scale
    masked = jnp.where(valid, scores, neg_fill)
    top = lax.optimization_barrier(jnp.max(masked, axis=1))
    weights = jnp.where(valid, jnp.exp(masked - top[:, None]), 0.0).astype(jnp.bfloat16)
    numer = jnp.dot(weights, keys[:, :LATENT], preferred_element_type=jnp.float32)
    total = lax.optimization_barrier(jnp.sum(weights.astype(jnp.float32), axis=1))
    return (numer, top, total)

def join(first, second):
    best = jnp.maximum(first[1], second[1])
    factor_a = jnp.exp(first[1] - best)
    factor_b = jnp.exp(second[1] - best)
    return (first[0] * factor_a[..., None] + second[0] * factor_b[..., None], best, first[2] * factor_a + second[2] * factor_b)

def reference(queries, cache, draft_latent, lengths, parents, value_up, out_proj):
    reach = tree_reach(parents)
    pieces = []
    for request in range(REQS):
        rows = queries[request].reshape(DRAFT * HEADS, LATENT + ROPE_DIM)
        blocks = cache[request].reshape(N_CTX, CTX_DEV, LATENT + ROPE_DIM)
        starts = jnp.arange(N_CTX, dtype=jnp.int32) * CTX_DEV
        limit = lengths[request]
        start_state = (jnp.zeros((DRAFT * HEADS, LATENT), jnp.float32), jnp.full((DRAFT * HEADS,), neg_fill, jnp.float32), jnp.zeros((DRAFT * HEADS,), jnp.float32))

        def fold(state, item):
            keys, first = item
            live = (first + jnp.arange(CTX_DEV, dtype=jnp.int32) < limit)[None, :]
            return (join(state, single_state(rows, keys, live)), None)
        state, unused = lax.scan(fold, start_state, (blocks, starts))
        tree = jnp.repeat(reach[request], HEADS, axis=0)
        state = join(state, single_state(rows, draft_latent[request], tree))
        latent_out = (state[0] / state[2][:, None]).astype(jnp.bfloat16).reshape(DRAFT, HEADS, LATENT)
        values = jnp.einsum('dhl,hlv->dhv', latent_out.astype(jnp.float32), value_up.astype(jnp.float32), precision=lax.Precision.HIGHEST).astype(jnp.bfloat16)
        pieces.append(values.reshape(DRAFT, HEADS * VALUE_DIM))
    flat = jnp.concatenate(pieces, axis=0)
    return jnp.dot(flat, out_proj, preferred_element_type=jnp.float32).astype(jnp.bfloat16)
```

```python
import math

import jax
import jax.numpy as jnp
from jax import lax
from jax.experimental import pallas as pl
from jax.experimental.pallas import tpu as pltpu
from jax.sharding import PartitionSpec as P

yarn_factor = 1.0 + 0.1 * math.log(32.0)
score_scale = yarn_factor * yarn_factor / math.sqrt(192.0)
log2_scale = score_scale / math.log(2.0)
neg_fill = -1e30
low_top = -1e29
PACK_ROWS = 8


VMEM = pl.BlockSpec(memory_space=pltpu.VMEM)
SMEM = pl.BlockSpec(memory_space=pltpu.SMEM)


def tree_bias(parents):
    drafts = parents.shape[0]
    order = jnp.arange(drafts, dtype=jnp.int32)
    step = (parents[:, None] == order[None, :]) | (order[:, None] == order[None, :])
    reach = step.astype(jnp.bfloat16)
    covered = 1
    while covered < drafts:
        grown = jnp.dot(reach, reach, preferred_element_type=jnp.float32)
        reach = (grown > 0.5).astype(jnp.bfloat16)
        covered *= 2
    return jnp.where(reach > 0.5, 0.0, neg_fill).astype(jnp.float32)


def scores_of(rows, keys):
    return (
        lax.dot_general(rows, keys, (((1,), (1,)), ((), ())), preferred_element_type=jnp.float32)
        * log2_scale
    )


def weigh(masked, keys, top, latent):
    weights = jnp.exp2(masked - top).astype(jnp.bfloat16)
    numer = jnp.dot(weights, keys[:, :latent], preferred_element_type=jnp.float32)
    return numer, jnp.sum(weights.astype(jnp.float32), axis=1, keepdims=True)


def position_bias(info_ref, slot, count):
    first = info_ref[slot]
    spot = first + lax.broadcasted_iota(jnp.int32, (1, count), 1)
    return jnp.where(spot < info_ref[0], 0.0, neg_fill)


def draft_kernel(q_ref, keys_ref, bias_ref, numer_ref, top_ref, total_ref):
    latent = numer_ref.shape[1]
    keys = keys_ref[...]
    repeats = q_ref.shape[0] // bias_ref.shape[0]
    bias = jnp.concatenate([bias_ref[...]] * repeats, axis=0)
    masked = scores_of(q_ref[...], keys) + bias
    top = jnp.max(masked, axis=1, keepdims=True)
    numer, total = weigh(masked, keys, top, latent)
    numer_ref[...] = numer
    top_ref[...] = top
    total_ref[...] = total


def fold(info_ref, rows, key_refs, slots, carry, latent):
    blocks, tops = [], []
    for key_ref, slot in zip(key_refs, slots):
        masked = scores_of(rows, key_ref[...]) + position_bias(info_ref, slot, key_ref.shape[0])
        blocks.append(masked)
        tops.append(jnp.max(masked, axis=1, keepdims=True))
    top = carry[1] if carry is not None else jnp.full_like(tops[0], low_top)
    for other in tops:
        top = jnp.maximum(top, other)
    numer = total = None
    if carry is not None:
        factor = jnp.exp2(carry[1] - top)
        numer, total = carry[0] * factor, carry[2] * factor
    for key_ref, masked in zip(key_refs, blocks):
        part, count = weigh(masked, key_ref[...], top, latent)
        numer = part if numer is None else numer + part
        total = count if total is None else total + count
    return numer, top, total


def first_kernel(peers, slots, info_ref, *refs):
    q_refs, refs = refs[:peers], refs[peers:]
    key_refs, (numer_ref, top_ref, total_ref) = refs[: len(slots)], refs[len(slots) :]
    rows = jnp.concatenate([q[...] for q in q_refs], axis=0)
    numer, top, total = fold(info_ref, rows, key_refs, slots, None, numer_ref.shape[1])
    numer_ref[...] = numer
    top_ref[...] = top
    total_ref[...] = total


def as_row(column):
    count = column.shape[0]
    eye = lax.broadcasted_iota(jnp.int32, (count, count), 0) == lax.broadcasted_iota(
        jnp.int32, (count, count), 1
    )
    return jnp.sum(jnp.where(eye, column, 0.0), axis=0, keepdims=True)


def as_column(row):
    count = row.shape[1]
    eye = lax.broadcasted_iota(jnp.int32, (count, count), 0) == lax.broadcasted_iota(
        jnp.int32, (count, count), 1
    )
    return jnp.sum(jnp.where(eye, row, 0.0), axis=1, keepdims=True)


def pieces(row):
    high = row.astype(jnp.bfloat16).astype(jnp.float32)
    rest = row - high
    middle = rest.astype(jnp.bfloat16).astype(jnp.float32)
    return [high, middle, rest - middle]


def last_kernel(peers, slots, info_ref, *refs):
    q_refs, refs = refs[:peers], refs[peers:]
    key_refs, refs = refs[: len(slots)], refs[len(slots) :]
    numer_ref, top_ref, total_ref = refs[:3]
    out_refs = refs[3:]
    rows = jnp.concatenate([q[...] for q in q_refs], axis=0)
    carry = (numer_ref[...], top_ref[...], total_ref[...])
    latent = numer_ref.shape[1]
    numer, top, total = fold(info_ref, rows, key_refs, slots, carry, latent)
    each = q_refs[0].shape[0]
    for peer, out_ref in enumerate(out_refs):
        here = slice(peer * each, (peer + 1) * each)
        out_ref[:each, :] = numer[here].astype(jnp.bfloat16)
        lines = pieces(as_row(top[here])) + pieces(as_row(total[here]))
        lines += [jnp.zeros_like(lines[0])] * (PACK_ROWS - len(lines))
        packed = jnp.concatenate(lines, axis=0)
        packed = jnp.concatenate(
            [packed, jnp.zeros((PACK_ROWS, latent - each), jnp.float32)], axis=1
        )
        out_ref[each:, :] = packed.astype(jnp.bfloat16)


def project_kernel(peers, info_ref, *refs):
    state_refs, refs = refs[:peers], refs[peers:]
    dnumer_ref, dtop_ref, dtotal_ref, up_ref, proj_ref, keep_ref, send_ref, flat_ref = refs
    each = dnumer_ref.shape[0]
    heads, latent, width = up_ref.shape
    drafts = each // heads
    tops, totals = [dtop_ref[...]], [dtotal_ref[...]]
    for state in state_refs:
        lines = state[each:, :each].astype(jnp.float32)
        tops.append(as_column(lines[0:1] + lines[1:2] + lines[2:3]))
        totals.append(as_column(lines[3:4] + lines[4:5] + lines[5:6]))
    best = tops[0]
    for other in tops[1:]:
        best = jnp.maximum(best, other)
    factor = jnp.exp2(tops[0] - best)
    numer, total = dnumer_ref[...] * factor, totals[0] * factor
    for state, top, count in zip(state_refs, tops[1:], totals[1:]):
        factor = jnp.exp2(top - best)
        numer = numer + state[:each, :].astype(jnp.float32) * factor
        total = total + count * factor
    latent_out = (numer / total).astype(jnp.bfloat16)
    for head in range(heads):
        value = jnp.dot(
            latent_out[head * drafts : (head + 1) * drafts],
            up_ref[head],
            preferred_element_type=jnp.float32,
        )
        flat_ref[:, head * width : (head + 1) * width] = value.astype(jnp.bfloat16)
    flat = flat_ref[...]
    columns = keep_ref.shape[2]
    span = math.lcm(2 * columns, 128)
    first_core = info_ref[1] == 0
    for block in range(proj_ref.shape[1] // span):
        part = jnp.dot(
            flat,
            proj_ref[:, block * span : (block + 1) * span],
            preferred_element_type=jnp.float32,
        )
        for pair in range(span // (2 * columns)):
            halves = []
            for side in range(2):
                shift = (2 * pair + side) * columns
                moved = part if shift == 0 else pltpu.roll(part, span - shift, 1)
                halves.append(moved[:, :columns])
            spot = block * (span // (2 * columns)) + pair
            keep_ref[spot] = jnp.where(first_core, halves[0], halves[1]).astype(jnp.bfloat16)
            send_ref[spot] = jnp.where(first_core, halves[1], halves[0]).astype(jnp.bfloat16)


def pair_kernel(info_ref, keep_ref, got_ref, own_ref, *out_refs):
    chip = info_ref[2]

    def both(spot):
        return keep_ref[spot].astype(jnp.float32) + got_ref[spot].astype(jnp.float32)

    for peer, out_ref in enumerate(out_refs):
        out_ref[...] = both(lax.bitwise_xor(chip, peer + 1)).astype(jnp.bfloat16)
    own_ref[...] = both(chip)


def call(kernel, outs, specs, scratch=(), limit=24, name=None):
    return pl.pallas_call(
        kernel,
        out_shape=outs,
        in_specs=specs,
        out_specs=jax.tree.map(lambda _: VMEM, outs),
        scratch_shapes=list(scratch),
        compiler_params=pltpu.CompilerParams(vmem_limit_bytes=limit << 20),
        name=name,
    )


def on_device(count, queries, cache, draft_latent, lengths, parents, value_up, out_proj):
    drafts, heads_here, width = queries.shape[1:]
    latent = value_up.shape[1]
    block_len = cache.shape[1]
    inner = 4
    outer = count // inner
    chips = count // 2
    columns = out_proj.shape[1] // count
    myself = lax.axis_index("ctx")
    starts = [lax.bitwise_xor(myself, bit) * block_len for bit in range(inner)]
    info = jnp.stack(
        [lengths[0], lax.rem(myself, 2), lax.div(myself, 2)] + starts
    ).astype(jnp.int32)

    def swap(value, bits):
        return lax.ppermute(value, "ctx", [(i, i ^ bits) for i in range(count)])

    keys_own = cache[0]
    keys_across = swap(keys_own, 2)
    keys_core = swap(keys_own, 1)
    own_rows = jnp.transpose(queries[0], (1, 0, 2)).reshape(heads_here * drafts, width)
    rows = [own_rows] + [swap(own_rows, inner * peer) for peer in range(1, outer)]
    keys_far = swap(keys_across, 1)

    each = heads_here * drafts
    f32, bf16 = jnp.float32, jnp.bfloat16
    dnumer, dtop, dtotal = call(
        draft_kernel,
        (
            jax.ShapeDtypeStruct((each, latent), f32),
            jax.ShapeDtypeStruct((each, 1), f32),
            jax.ShapeDtypeStruct((each, 1), f32),
        ),
        [VMEM] * 3,
        name="draft",
    )(own_rows, draft_latent[0], tree_bias(parents[0]))

    def first(*args):
        return first_kernel(outer, (3, 4), *args)

    state = call(
        first,
        (
            jax.ShapeDtypeStruct((outer * each, latent), f32),
            jax.ShapeDtypeStruct((outer * each, 1), f32),
            jax.ShapeDtypeStruct((outer * each, 1), f32),
        ),
        [SMEM] + [VMEM] * (outer + 2),
        name="first",
    )(info, *rows, keys_own, keys_core)

    def last(*args):
        return last_kernel(outer, (5, 6), *args)

    states = call(
        last,
        tuple(jax.ShapeDtypeStruct((each + PACK_ROWS, latent), bf16) for _ in range(outer)),
        [SMEM] + [VMEM] * (outer + 5),
        name="last",
    )(info, *rows, keys_across, keys_far, *state)
    got = [states[0]] + [swap(states[peer], inner * peer) for peer in range(outer - 1, 0, -1)]

    def project(*args):
        return project_kernel(outer, *args)

    keep, send = call(
        project,
        tuple(jax.ShapeDtypeStruct((chips, drafts, columns), bf16) for _ in range(2)),
        [SMEM] + [VMEM] * (outer + 5),
        scratch=[pltpu.VMEM((drafts, heads_here * value_up.shape[2]), bf16)],
        name="project",
    )(info, *got, dnumer, dtop, dtotal, value_up, out_proj)
    other = swap(send, 1)
    own, *parts = call(
        pair_kernel,
        (jax.ShapeDtypeStruct((drafts, columns), f32),)
        + tuple(jax.ShapeDtypeStruct((drafts, columns), bf16) for _ in range(chips - 1)),
        [SMEM] + [VMEM] * 2,
        name="pair",
    )(info, keep, other)
    result = own
    for peer in range(chips - 1, 0, -1):
        result = result + swap(parts[peer - 1], 2 * peer).astype(f32)
    return result.astype(bf16)


def solution(mesh):
    in_specs = (
        P("grp", None, "ctx", None),
        P("grp", "ctx", None),
        P("grp", None, None),
        P("grp"),
        P("grp", None),
        P("ctx", None, None),
        P("ctx", None),
    )
    count = mesh.shape["ctx"]

    def body(*args):
        return on_device(count, *args)

    return jax.shard_map(
        body, mesh=mesh, in_specs=in_specs, out_specs=P("grp", "ctx"), check_vma=False
    )
```

```python
import math

import jax
import jax.numpy as jnp
from jax import lax
from jax.experimental import pallas as pl
from jax.experimental.pallas import tpu as pltpu
from jax.sharding import PartitionSpec as P


yarn_factor = 1.0 + 0.1 * math.log(32.0)
score_scale = yarn_factor * yarn_factor / math.sqrt(192.0)
log2_scale = score_scale / math.log(2.0)
neg_fill = -1e30
low_top = -1e29
PACK_ROWS = 8


def tree_bias(parents):
    drafts = parents.shape[0]
    order = jnp.arange(drafts, dtype=jnp.int32)
    step = (parents[:, None] == order[None, :]) | (order[:, None] == order[None, :])
    reach = step.astype(jnp.bfloat16)
    covered = 1
    while covered < drafts:
        grown = jnp.dot(reach, reach, preferred_element_type=jnp.float32)
        reach = (grown > 0.5).astype(jnp.bfloat16)
        covered *= 2
    return jnp.where(reach > 0.5, 0.0, neg_fill).astype(jnp.float32)


NT = (((1,), (1,)), ((), ()))


def weights_of(masked, top):
    weights = jnp.exp2(masked - top).astype(jnp.bfloat16)
    return weights, jnp.sum(weights.astype(jnp.float32), axis=1, keepdims=True)


def draft_kernel(q_ref, keys_ref, bias_ref, up_from, numer_ref, top_ref, total_ref, up_ref):
    up_ref[...] = up_from[...]
    latent = numer_ref.shape[1]
    keys = keys_ref[...]
    repeats = q_ref.shape[0] // bias_ref.shape[0]
    bias = jnp.concatenate([bias_ref[...]] * repeats, axis=0)
    scores = lax.dot_general(q_ref[...], keys, NT, preferred_element_type=jnp.float32)
    masked = scores * log2_scale + bias
    top = jnp.max(masked, axis=1, keepdims=True)
    weights, total = weights_of(masked, top)
    numer_ref[...] = jnp.dot(weights, keys[:, :latent], preferred_element_type=jnp.float32)
    top_ref[...] = top
    total_ref[...] = total


def fold(rows, key_refs, bias_ref, carry, latent):
    blocks, tops = [], []
    for spot, key_ref in enumerate(key_refs):
        scores = jnp.dot(rows, key_ref[...], preferred_element_type=jnp.float32)
        masked = scores * log2_scale + bias_ref[spot : spot + 1, :]
        blocks.append(masked)
        tops.append(jnp.max(masked, axis=1, keepdims=True))
    top = carry[1] if carry is not None else jnp.full_like(tops[0], low_top)
    for other in tops:
        top = jnp.maximum(top, other)
    numer = total = None
    if carry is not None:
        factor = jnp.exp2(carry[1] - top)
        numer, total = carry[0] * factor, carry[2] * factor
    for key_ref, masked in zip(key_refs, blocks):
        weights, count = weights_of(masked, top)
        part = lax.dot_general(weights, key_ref[:latent, :], NT, preferred_element_type=jnp.float32)
        numer = part if numer is None else numer + part
        total = count if total is None else total + count
    return numer, top, total


def join_rows(q_refs):
    return jnp.concatenate([q[...] for q in q_refs], axis=0)


def first_kernel(peers, bias_ref, *refs):
    q_refs, refs = refs[:peers], refs[peers:]
    key_refs, (numer_ref, top_ref, total_ref) = refs[:-3], refs[-3:]
    numer, top, total = fold(join_rows(q_refs), key_refs, bias_ref, None, numer_ref.shape[1])
    numer_ref[...] = numer
    top_ref[...] = top
    total_ref[...] = total


def middle_kernel(peers, bias_ref, *refs):
    q_refs, (key_ref, *carry_refs, numer_ref, top_ref, total_ref) = refs[:peers], refs[peers:]
    carry = tuple(ref[...] for ref in carry_refs)
    numer, top, total = fold(join_rows(q_refs), [key_ref], bias_ref, carry, numer_ref.shape[1])
    numer_ref[...] = numer
    top_ref[...] = top
    total_ref[...] = total


def as_row(column):
    count = column.shape[0]
    eye = lax.broadcasted_iota(jnp.int32, (count, count), 0) == lax.broadcasted_iota(
        jnp.int32, (count, count), 1
    )
    return jnp.sum(jnp.where(eye, column, 0.0), axis=0, keepdims=True)


def as_column(row):
    count = row.shape[1]
    eye = lax.broadcasted_iota(jnp.int32, (count, count), 0) == lax.broadcasted_iota(
        jnp.int32, (count, count), 1
    )
    return jnp.sum(jnp.where(eye, row, 0.0), axis=1, keepdims=True)


def pieces(row):
    high = row.astype(jnp.bfloat16).astype(jnp.float32)
    rest = row - high
    middle = rest.astype(jnp.bfloat16).astype(jnp.float32)
    return [high, middle, rest - middle]


def last_kernel(peers, bias_ref, *refs):
    q_refs, (key_ref, *rest) = refs[:peers], refs[peers:]
    numer_ref, top_ref, total_ref, own_refs, out_refs = *rest[:3], rest[3:6], rest[6:]
    carry = (numer_ref[...], top_ref[...], total_ref[...])
    latent = numer_ref.shape[1]
    numer, top, total = fold(join_rows(q_refs), [key_ref], bias_ref, carry, latent)
    each = q_refs[0].shape[0]
    for own_ref, value in zip(own_refs, (numer, top, total)):
        own_ref[...] = value[:each]
    for peer, out_ref in enumerate(out_refs, 1):
        here = slice(peer * each, (peer + 1) * each)
        out_ref[:each, :] = numer[here].astype(jnp.bfloat16)
        lines = pieces(as_row(top[here])) + pieces(as_row(total[here]))
        lines += [jnp.zeros_like(lines[0])] * (PACK_ROWS - len(lines))
        packed = jnp.concatenate(lines, axis=0)
        packed = jnp.concatenate(
            [packed, jnp.zeros((PACK_ROWS, latent - each), jnp.float32)], axis=1
        )
        out_ref[each:, :] = packed.astype(jnp.bfloat16)


def project_kernel(peers, *refs):
    state_refs, refs = refs[: peers - 1], refs[peers - 1 :]
    full_refs, refs = refs[:6], refs[6:]
    up_ref, proj_from, keep_ref, send_ref, flat_ref, proj_ref, done = refs
    each = full_refs[0].shape[0]
    heads, _, width = up_ref.shape
    columns = keep_ref.shape[2]
    span = math.lcm(2 * columns, 128)
    blocks = proj_ref.shape[1] // span
    copies = []
    for block in range(blocks):
        strip = (slice(None), pl.ds(block * span, span))
        copies.append(
            pltpu.make_async_copy(proj_from.at[strip], proj_ref.at[strip], done.at[block])
        )
    for copy in copies:
        copy.start()
    drafts = each // heads
    numers = [full_refs[0][...], full_refs[3][...]]
    tops = [full_refs[1][...], full_refs[4][...]]
    totals = [full_refs[2][...], full_refs[5][...]]
    for state in state_refs:
        lines = state[each:, :each].astype(jnp.float32)
        numers.append(state[:each, :].astype(jnp.float32))
        tops.append(as_column(lines[0:1] + lines[1:2] + lines[2:3]))
        totals.append(as_column(lines[3:4] + lines[4:5] + lines[5:6]))
    best = tops[0]
    for other in tops[1:]:
        best = jnp.maximum(best, other)
    numer = total = 0.0
    for part, top, count in zip(numers, tops, totals):
        factor = jnp.exp2(top - best)
        numer = numer + part * factor
        total = total + count * factor
    latent_out = (numer / total).astype(jnp.bfloat16)
    for head in range(heads):
        value = jnp.dot(
            latent_out[head * drafts : (head + 1) * drafts],
            up_ref[head],
            preferred_element_type=jnp.float32,
        )
        flat_ref[:, head * width : (head + 1) * width] = value.astype(jnp.bfloat16)
    flat = flat_ref[...]
    first_core = lax.rem(lax.axis_index("ctx"), 2) == 0
    for block in range(blocks):
        copies[block].wait()
        part = jnp.dot(
            flat,
            proj_ref[:, block * span : (block + 1) * span],
            preferred_element_type=jnp.float32,
        )
        for pair in range(span // (2 * columns)):
            halves = []
            for side in range(2):
                shift = (2 * pair + side) * columns
                moved = part if shift == 0 else pltpu.roll(part, span - shift, 1)
                halves.append(moved[:, :columns])
            spot = block * (span // (2 * columns)) + pair
            keep_ref[spot] = jnp.where(first_core, halves[0], halves[1])
            send_ref[spot] = jnp.where(first_core, halves[1], halves[0]).astype(jnp.bfloat16)


def pair_kernel(keep_ref, got_ref, stay_ref, send_ref):
    side = lax.rem(lax.div(lax.axis_index("ctx"), 2), 2)
    for spot in range(stay_ref.shape[0]):
        mine = 2 * spot + side
        yours = 2 * spot + 1 - side
        stay_ref[spot] = keep_ref[mine] + got_ref[mine].astype(jnp.float32)
        send_ref[spot] = (keep_ref[yours] + got_ref[yours].astype(jnp.float32)).astype(jnp.bfloat16)


def quad_kernel(stay_ref, got_ref, own_ref, *out_refs):
    outer = lax.div(lax.axis_index("ctx"), 4)

    def both(spot):
        return stay_ref[spot] + got_ref[spot].astype(jnp.float32)

    for peer, out_ref in enumerate(out_refs, 1):
        out_ref[...] = both(lax.bitwise_xor(outer, peer)).astype(jnp.bfloat16)
    own_ref[...] = both(outer)


def call(kernel, outs, values, specs=None, scratch=(), limit=24):
    return pl.pallas_call(
        kernel,
        out_shape=outs,
        in_specs=specs or [pl.BlockSpec() for _ in values],
        scratch_shapes=list(scratch),
        compiler_params=pltpu.CompilerParams(vmem_limit_bytes=limit << 20),
    )(*values)


def shaped(*shape, dtype=jnp.float32):
    return jax.ShapeDtypeStruct(shape, dtype)


def on_device(count, queries, cache, draft_latent, lengths, parents, value_up, out_proj):
    drafts, heads_here, width = queries.shape[1:]
    latent = value_up.shape[1]
    block_len = cache.shape[1]
    inner = 4
    outer = count // inner
    chips = count // 2
    columns = out_proj.shape[1] // count
    each = heads_here * drafts
    bf16 = jnp.bfloat16
    myself = lax.axis_index("ctx")

    def bias_of(*bits):
        firsts = jnp.stack([lax.bitwise_xor(myself, bit) * block_len for bit in bits])
        spots = firsts[:, None] + jnp.arange(block_len, dtype=jnp.int32)[None, :]
        return jnp.where(spots < lengths[0], 0.0, neg_fill).astype(jnp.float32)

    def swap(value, bits):
        return lax.ppermute(value, "ctx", [(i, i ^ bits) for i in range(count)])

    keys_own = jnp.transpose(cache[0])
    keys_across = swap(keys_own, 2)
    keys_core = swap(keys_own, 1)
    own_rows = jnp.transpose(queries[0], (1, 0, 2)).reshape(each, width)
    rows = [own_rows] + [swap(own_rows, inner * peer) for peer in range(outer - 1, 0, -1)][::-1]
    keys_far = swap(keys_across, 1)

    state_shape = (shaped(outer * each, latent), shaped(outer * each, 1), shaped(outer * each, 1))
    own_shape = (shaped(each, latent), shaped(each, 1), shaped(each, 1))
    *drafted, up_here = call(
        draft_kernel,
        own_shape + (shaped(*value_up.shape, dtype=bf16),),
        (own_rows, draft_latent[0], tree_bias(parents[0]), value_up),
    )
    state = call(
        lambda *refs: first_kernel(outer, *refs),
        state_shape,
        (bias_of(0, 1), *rows, keys_own, keys_core),
    )
    state = call(
        lambda *refs: middle_kernel(outer, *refs),
        state_shape,
        (bias_of(2), *rows, keys_across, *state),
    )
    done = call(
        lambda *refs: last_kernel(outer, *refs),
        own_shape
        + tuple(shaped(each + PACK_ROWS, latent, dtype=bf16) for _ in range(outer - 1)),
        (bias_of(3), *rows, keys_far, *state),
    )
    whole, states = done[:3], done[3:]
    got = [swap(states[peer - 1], inner * peer) for peer in range(outer - 1, 0, -1)]
    keep, send = call(
        lambda *refs: project_kernel(outer, *refs),
        (shaped(chips, drafts, columns), shaped(chips, drafts, columns, dtype=bf16)),
        (*got, *whole, *drafted, up_here, out_proj),
        specs=[pl.BlockSpec()] * (outer + 6) + [pl.BlockSpec(memory_space=pl.ANY)],
        scratch=[
            pltpu.VMEM((drafts, heads_here * value_up.shape[2]), bf16),
            pltpu.VMEM(out_proj.shape, bf16),
            pltpu.SemaphoreType.DMA((out_proj.shape[1] // math.lcm(2 * columns, 128),)),
        ],
        limit=50,
    )
    stay, send = call(
        pair_kernel,
        (shaped(chips // 2, drafts, columns), shaped(chips // 2, drafts, columns, dtype=bf16)),
        (keep, swap(send, 1)),
    )
    own, *parts = call(
        quad_kernel,
        (shaped(drafts, columns),)
        + tuple(shaped(drafts, columns, dtype=bf16) for _ in range(outer - 1)),
        (stay, swap(send, 2)),
    )
    result = own
    for peer in range(outer - 1, 0, -1):
        result = result + swap(parts[peer - 1], inner * peer).astype(jnp.float32)
    return result.astype(bf16)


def solution(mesh):
    in_specs = (
        P("grp", None, "ctx", None),
        P("grp", "ctx", None),
        P("grp", None, None),
        P("grp"),
        P("grp", None),
        P("ctx", None, None),
        P("ctx", None),
    )
    count = mesh.shape["ctx"]

    def body(*args):
        return on_device(count, *args)

    return jax.shard_map(
        body, mesh=mesh, in_specs=in_specs, out_specs=P("grp", "ctx"), check_vma=False
    )
```

```python
import math

import jax
import jax.numpy as jnp
from jax import lax
from jax.experimental import pallas as pl
from jax.experimental.pallas import tpu as pltpu
from jax.sharding import PartitionSpec as P


yarn_factor = 1.0 + 0.1 * math.log(32.0)
score_scale = yarn_factor * yarn_factor / math.sqrt(192.0)
log2_scale = score_scale / math.log(2.0)
neg_fill = -1e30
low_top = -1e29
PACK_ROWS = 8


NT = (((1,), (1,)), ((), ()))


def weights_of(masked, top):
    weights = jnp.exp2(masked - top).astype(jnp.bfloat16)
    return weights, jnp.sum(weights.astype(jnp.float32), axis=1, keepdims=True)


def as_row(column):
    count = column.shape[0]
    eye = lax.broadcasted_iota(jnp.int32, (count, count), 0) == lax.broadcasted_iota(
        jnp.int32, (count, count), 1
    )
    return jnp.sum(jnp.where(eye, column, 0.0), axis=0, keepdims=True)


def as_column(row):
    count = row.shape[1]
    eye = lax.broadcasted_iota(jnp.int32, (count, count), 0) == lax.broadcasted_iota(
        jnp.int32, (count, count), 1
    )
    return jnp.sum(jnp.where(eye, row, 0.0), axis=1, keepdims=True)


def tree_bias(parents):
    drafts = parents.shape[1]
    order = lax.broadcasted_iota(jnp.int32, (drafts, drafts), 1)
    self_order = lax.broadcasted_iota(jnp.int32, (drafts, drafts), 0)
    parent = as_column(parents.astype(jnp.float32)).astype(jnp.int32)
    reach = jnp.where((parent == order) | (self_order == order), 1.0, 0.0)
    covered = 1
    while covered < drafts:
        step = reach.astype(jnp.bfloat16)
        grown = jnp.dot(step, step, preferred_element_type=jnp.float32)
        reach = jnp.where(grown > 0.5, 1.0, 0.0)
        covered *= 2
    return jnp.where(reach > 0.5, 0.0, neg_fill)


def draft_kernel(
    q_ref, keys_ref, parents_ref, up_from, numer_ref, top_ref, total_ref, up_ref
):
    up_ref[...] = up_from[...]
    latent = numer_ref.shape[1]
    keys = keys_ref[...]
    repeats = q_ref.shape[0] // keys.shape[0]
    bias = jnp.concatenate([tree_bias(parents_ref[...])] * repeats, axis=0)
    scores = lax.dot_general(q_ref[...], keys, NT, preferred_element_type=jnp.float32)
    masked = scores * log2_scale + bias
    top = jnp.max(masked, axis=1, keepdims=True)
    weights, total = weights_of(masked, top)
    numer_ref[...] = jnp.dot(weights, keys[:, :latent], preferred_element_type=jnp.float32)
    top_ref[...] = top
    total_ref[...] = total


def fold(rows, key_refs, bias_ref, carry, latent):
    blocks, tops = [], []
    for spot, key_ref in enumerate(key_refs):
        scores = jnp.dot(rows, key_ref[...], preferred_element_type=jnp.float32)
        masked = scores * log2_scale + bias_ref[spot : spot + 1, :]
        blocks.append(masked)
        tops.append(jnp.max(masked, axis=1, keepdims=True))
    top = carry[1] if carry is not None else jnp.full_like(tops[0], low_top)
    for other in tops:
        top = jnp.maximum(top, other)
    numer = total = None
    if carry is not None:
        factor = jnp.exp2(carry[1] - top)
        numer, total = carry[0] * factor, carry[2] * factor
    for key_ref, masked in zip(key_refs, blocks):
        weights, count = weights_of(masked, top)
        part = lax.dot_general(weights, key_ref[:latent, :], NT, preferred_element_type=jnp.float32)
        numer = part if numer is None else numer + part
        total = count if total is None else total + count
    return numer, top, total


def join_rows(q_refs):
    return jnp.concatenate([q[...] for q in q_refs], axis=0)


def first_kernel(peers, bias_ref, *refs):
    q_refs, refs = refs[:peers], refs[peers:]
    key_refs, (numer_ref, top_ref, total_ref) = refs[:-3], refs[-3:]
    numer, top, total = fold(join_rows(q_refs), key_refs, bias_ref, None, numer_ref.shape[1])
    numer_ref[...] = numer
    top_ref[...] = top
    total_ref[...] = total


def middle_kernel(peers, bias_ref, *refs):
    q_refs, (key_ref, *carry_refs, numer_ref, top_ref, total_ref) = refs[:peers], refs[peers:]
    carry = tuple(ref[...] for ref in carry_refs)
    numer, top, total = fold(join_rows(q_refs), [key_ref], bias_ref, carry, numer_ref.shape[1])
    numer_ref[...] = numer
    top_ref[...] = top
    total_ref[...] = total


def pieces(row):
    high = row.astype(jnp.bfloat16).astype(jnp.float32)
    rest = row - high
    middle = rest.astype(jnp.bfloat16).astype(jnp.float32)
    return [high, middle, rest - middle]


def last_kernel(peers, bias_ref, *refs):
    q_refs, (key_ref, *rest) = refs[:peers], refs[peers:]
    numer_ref, top_ref, total_ref, own_refs, out_refs = *rest[:3], rest[3:6], rest[6:]
    carry = (numer_ref[...], top_ref[...], total_ref[...])
    latent = numer_ref.shape[1]
    numer, top, total = fold(join_rows(q_refs), [key_ref], bias_ref, carry, latent)
    each = q_refs[0].shape[0]
    for own_ref, value in zip(own_refs, (numer, top, total)):
        own_ref[...] = value[:each]
    for peer, out_ref in enumerate(out_refs, 1):
        here = slice(peer * each, (peer + 1) * each)
        out_ref[:each, :] = numer[here].astype(jnp.bfloat16)
        lines = pieces(as_row(top[here])) + pieces(as_row(total[here]))
        lines += [jnp.zeros_like(lines[0])] * (PACK_ROWS - len(lines))
        packed = jnp.concatenate(lines, axis=0)
        packed = jnp.concatenate(
            [packed, jnp.zeros((PACK_ROWS, latent - each), jnp.float32)], axis=1
        )
        out_ref[each:, :] = packed.astype(jnp.bfloat16)


def project_kernel(peers, *refs):
    state_refs, refs = refs[: peers - 1], refs[peers - 1 :]
    full_refs, refs = refs[:6], refs[6:]
    up_ref, proj_ref, keep_ref, send_ref, flat_ref = refs
    each = full_refs[0].shape[0]
    heads, _, width = up_ref.shape
    columns = keep_ref.shape[2]
    span = math.lcm(2 * columns, 128)
    blocks = proj_ref.shape[1] // span
    drafts = each // heads
    numers = [full_refs[0][...], full_refs[3][...]]
    tops = [full_refs[1][...], full_refs[4][...]]
    totals = [full_refs[2][...], full_refs[5][...]]
    for state in state_refs:
        lines = state[each:, :each].astype(jnp.float32)
        numers.append(state[:each, :].astype(jnp.float32))
        tops.append(as_column(lines[0:1] + lines[1:2] + lines[2:3]))
        totals.append(as_column(lines[3:4] + lines[4:5] + lines[5:6]))
    best = tops[0]
    for other in tops[1:]:
        best = jnp.maximum(best, other)
    numer = total = 0.0
    for part, top, count in zip(numers, tops, totals):
        factor = jnp.exp2(top - best)
        numer = numer + part * factor
        total = total + count * factor
    latent_out = (numer / total).astype(jnp.bfloat16)
    for head in range(heads):
        value = jnp.dot(
            latent_out[head * drafts : (head + 1) * drafts],
            up_ref[head],
            preferred_element_type=jnp.float32,
        )
        flat_ref[:, head * width : (head + 1) * width] = value.astype(jnp.bfloat16)
    flat = flat_ref[...]
    first_core = lax.rem(lax.axis_index("ctx"), 2) == 0
    for block in range(blocks):
        part = jnp.dot(
            flat,
            proj_ref[:, block * span : (block + 1) * span],
            preferred_element_type=jnp.float32,
        )
        for pair in range(span // (2 * columns)):
            halves = []
            for side in range(2):
                shift = (2 * pair + side) * columns
                moved = part if shift == 0 else pltpu.roll(part, span - shift, 1)
                halves.append(moved[:, :columns])
            spot = block * (span // (2 * columns)) + pair
            keep_ref[spot] = jnp.where(first_core, halves[0], halves[1])
            send_ref[spot] = jnp.where(first_core, halves[1], halves[0]).astype(jnp.bfloat16)


def pair_kernel(keep_ref, got_ref, stay_ref, send_ref):
    side = lax.rem(lax.div(lax.axis_index("ctx"), 2), 2)
    for spot in range(stay_ref.shape[0]):
        mine = 2 * spot + side
        yours = 2 * spot + 1 - side
        stay_ref[spot] = keep_ref[mine] + got_ref[mine].astype(jnp.float32)
        send_ref[spot] = (keep_ref[yours] + got_ref[yours].astype(jnp.float32)).astype(jnp.bfloat16)


def quad_kernel(stay_ref, got_ref, own_ref, *out_refs):
    outer = lax.div(lax.axis_index("ctx"), 4)

    def both(spot):
        return stay_ref[spot] + got_ref[spot].astype(jnp.float32)

    for peer, out_ref in enumerate(out_refs, 1):
        out_ref[...] = both(lax.bitwise_xor(outer, peer)).astype(jnp.bfloat16)
    own_ref[...] = both(outer)


def call(kernel, outs, values, specs=None, out_specs=None, scratch=(), limit=24):
    return pl.pallas_call(
        kernel,
        out_shape=outs,
        in_specs=specs or [pl.BlockSpec() for _ in values],
        out_specs=out_specs or [pl.BlockSpec() for _ in outs],
        scratch_shapes=list(scratch),
        compiler_params=pltpu.CompilerParams(vmem_limit_bytes=limit << 20),
    )(*values)


def shaped(*shape, dtype=jnp.float32):
    return jax.ShapeDtypeStruct(shape, dtype)


def on_device(count, queries, cache, draft_latent, lengths, parents, value_up, out_proj):
    drafts, heads_here, width = queries.shape[1:]
    latent = value_up.shape[1]
    block_len = cache.shape[1]
    inner = 4
    outer = count // inner
    chips = count // 2
    columns = out_proj.shape[1] // count
    each = heads_here * drafts
    bf16 = jnp.bfloat16
    myself = lax.axis_index("ctx")

    def bias_of(*bits):
        firsts = jnp.stack([lax.bitwise_xor(myself, bit) * block_len for bit in bits])
        spots = firsts[:, None] + jnp.arange(block_len, dtype=jnp.int32)[None, :]
        return jnp.where(spots < lengths[0], 0.0, neg_fill).astype(jnp.float32)

    def swap(value, bits):
        return lax.ppermute(value, "ctx", [(i, i ^ bits) for i in range(count)])

    keys_own = jnp.transpose(cache[0])
    keys_across = swap(keys_own, 2)
    keys_core = swap(keys_own, 1)
    own_rows = jnp.transpose(queries[0], (1, 0, 2)).reshape(each, width)
    rows = {0: own_rows}
    bit = outer // 2
    while bit:
        for peer in list(rows):
            rows[peer ^ bit] = swap(rows[peer], inner * bit)
        bit //= 2
    rows = [rows[peer] for peer in range(outer)]
    keys_far = swap(keys_across, 1)

    state_shape = (shaped(outer * each, latent), shaped(outer * each, 1), shaped(outer * each, 1))
    own_shape = (shaped(each, latent), shaped(each, 1), shaped(each, 1))
    proj_here = jnp.where(lengths[0] > -1, out_proj, jnp.zeros_like(out_proj))
    *drafted, up_here = call(
        draft_kernel,
        own_shape + (shaped(*value_up.shape, dtype=bf16),),
        (own_rows, draft_latent[0], parents, value_up),
    )
    state = call(
        lambda *refs: first_kernel(outer, *refs),
        state_shape,
        (bias_of(0, 1), *rows, keys_own, keys_core),
    )
    state = call(
        lambda *refs: middle_kernel(outer, *refs),
        state_shape,
        (bias_of(2), *rows, keys_across, *state),
    )
    done = call(
        lambda *refs: last_kernel(outer, *refs),
        own_shape
        + tuple(shaped(each + PACK_ROWS, latent, dtype=bf16) for _ in range(outer - 1)),
        (bias_of(3), *rows, keys_far, *state),
    )
    whole, states = done[:3], done[3:]
    got = [swap(states[peer - 1], inner * peer) for peer in range(outer - 1, 0, -1)]
    keep, send = call(
        lambda *refs: project_kernel(outer, *refs),
        (shaped(chips, drafts, columns), shaped(chips, drafts, columns, dtype=bf16)),
        (*got, *whole, *drafted, up_here, proj_here),
        scratch=[pltpu.VMEM((drafts, heads_here * value_up.shape[2]), bf16)],
    )
    stay, send = call(
        pair_kernel,
        (shaped(chips // 2, drafts, columns), shaped(chips // 2, drafts, columns, dtype=bf16)),
        (keep, swap(send, 1)),
    )
    own, *parts = call(
        quad_kernel,
        (shaped(drafts, columns),)
        + tuple(shaped(drafts, columns, dtype=bf16) for _ in range(outer - 1)),
        (stay, swap(send, 2)),
    )
    result = own
    for peer in range(outer - 1, 0, -1):
        result = result + swap(parts[peer - 1], inner * peer).astype(jnp.float32)
    return result.astype(bf16)


def solution(mesh):
    in_specs = (
        P("grp", None, "ctx", None),
        P("grp", "ctx", None),
        P("grp", None, None),
        P("grp"),
        P("grp", None),
        P("ctx", None, None),
        P("ctx", None),
    )
    count = mesh.shape["ctx"]

    def body(*args):
        return on_device(count, *args)

    return jax.shard_map(
        body, mesh=mesh, in_specs=in_specs, out_specs=P("grp", "ctx"), check_vma=False
    )
```

```python
import math

import jax
import jax.numpy as jnp
from jax import lax
from jax.experimental import pallas as pl
from jax.experimental.pallas import tpu as pltpu
from jax.sharding import PartitionSpec as P


yarn_factor = 1.0 + 0.1 * math.log(32.0)
score_scale = yarn_factor * yarn_factor / math.sqrt(192.0)
log2_scale = score_scale / math.log(2.0)
neg_fill = -1e30
low_top = -1e29
PACK_ROWS = 8


NT = (((1,), (1,)), ((), ()))


def weights_of(masked, top):
    weights = jnp.exp2(masked - top).astype(jnp.bfloat16)
    return weights, jnp.sum(weights.astype(jnp.float32), axis=1, keepdims=True)


def as_row(column):
    count = column.shape[0]
    eye = lax.broadcasted_iota(jnp.int32, (count, count), 0) == lax.broadcasted_iota(
        jnp.int32, (count, count), 1
    )
    return jnp.sum(jnp.where(eye, column, 0.0), axis=0, keepdims=True)


def as_column(row):
    count = row.shape[1]
    eye = lax.broadcasted_iota(jnp.int32, (count, count), 0) == lax.broadcasted_iota(
        jnp.int32, (count, count), 1
    )
    return jnp.sum(jnp.where(eye, row, 0.0), axis=1, keepdims=True)


def tree_bias(parents):
    drafts = parents.shape[1]
    order = lax.broadcasted_iota(jnp.int32, (drafts, drafts), 1)
    self_order = lax.broadcasted_iota(jnp.int32, (drafts, drafts), 0)
    parent = as_column(parents.astype(jnp.float32)).astype(jnp.int32)
    reach = jnp.where((parent == order) | (self_order == order), 1.0, 0.0)
    covered = 1
    while covered < drafts:
        step = reach.astype(jnp.bfloat16)
        grown = jnp.dot(step, step, preferred_element_type=jnp.float32)
        reach = jnp.where(grown > 0.5, 1.0, 0.0)
        covered *= 2
    return jnp.where(reach > 0.5, 0.0, neg_fill)


def draft_kernel(
    q_ref, keys_ref, parents_ref, up_from, numer_ref, top_ref, total_ref, up_ref
):
    up_ref[...] = up_from[...]
    latent = numer_ref.shape[1]
    keys = keys_ref[...]
    repeats = q_ref.shape[0] // keys.shape[0]
    bias = jnp.concatenate([tree_bias(parents_ref[...])] * repeats, axis=0)
    scores = lax.dot_general(q_ref[...], keys, NT, preferred_element_type=jnp.float32)
    masked = scores * log2_scale + bias
    top = jnp.max(masked, axis=1, keepdims=True)
    weights, total = weights_of(masked, top)
    numer_ref[...] = jnp.dot(weights, keys[:, :latent], preferred_element_type=jnp.float32)
    top_ref[...] = top
    total_ref[...] = total


def fold(rows, key_refs, bias_ref, carry, latent):
    blocks, tops = [], []
    at = 0
    for key_ref in key_refs:
        scores = jnp.dot(rows, key_ref[...], preferred_element_type=jnp.float32)
        masked = scores * log2_scale + bias_ref[:, at : at + key_ref.shape[1]]
        at += key_ref.shape[1]
        blocks.append(masked)
        tops.append(jnp.max(masked, axis=1, keepdims=True))
    top = carry[1] if carry is not None else jnp.full_like(tops[0], low_top)
    for other in tops:
        top = jnp.maximum(top, other)
    numer = total = None
    if carry is not None:
        factor = jnp.exp2(carry[1] - top)
        numer, total = carry[0] * factor, carry[2] * factor
    for key_ref, masked in zip(key_refs, blocks):
        weights, count = weights_of(masked, top)
        part = lax.dot_general(weights, key_ref[:latent, :], NT, preferred_element_type=jnp.float32)
        numer = part if numer is None else numer + part
        total = count if total is None else total + count
    return numer, top, total


def join_rows(q_refs):
    return jnp.concatenate([q[...] for q in q_refs], axis=0)


def first_kernel(peers, bias_ref, *refs):
    q_refs, refs = refs[:peers], refs[peers:]
    key_refs, (numer_ref, top_ref, total_ref) = refs[:-3], refs[-3:]
    numer, top, total = fold(join_rows(q_refs), key_refs, bias_ref, None, numer_ref.shape[1])
    numer_ref[...] = numer
    top_ref[...] = top
    total_ref[...] = total


def middle_kernel(peers, bias_ref, *refs):
    q_refs, refs = refs[:peers], refs[peers:]
    key_refs, carry_refs, out_refs = refs[:-6], refs[-6:-3], refs[-3:]
    carry = tuple(ref[...] for ref in carry_refs)
    state = fold(join_rows(q_refs), key_refs, bias_ref, carry, out_refs[0].shape[1])
    for out_ref, value in zip(out_refs, state):
        out_ref[...] = value


def pieces(row):
    high = row.astype(jnp.bfloat16).astype(jnp.float32)
    rest = row - high
    middle = rest.astype(jnp.bfloat16).astype(jnp.float32)
    return [high, middle, rest - middle]


def last_kernel(peers, bias_ref, *refs):
    q_refs, (key_ref, *rest) = refs[:peers], refs[peers:]
    numer_ref, top_ref, total_ref, own_refs, out_refs = *rest[:3], rest[3:6], rest[6:]
    carry = (numer_ref[...], top_ref[...], total_ref[...])
    latent = numer_ref.shape[1]
    numer, top, total = fold(join_rows(q_refs), [key_ref], bias_ref, carry, latent)
    each = q_refs[0].shape[0]
    for own_ref, value in zip(own_refs, (numer, top, total)):
        own_ref[...] = value[:each]
    for peer, out_ref in enumerate(out_refs, 1):
        here = slice(peer * each, (peer + 1) * each)
        out_ref[:each, :] = numer[here].astype(jnp.bfloat16)
        lines = pieces(as_row(top[here])) + pieces(as_row(total[here]))
        lines += [jnp.zeros_like(lines[0])] * (PACK_ROWS - len(lines))
        packed = jnp.concatenate(lines, axis=0)
        packed = jnp.concatenate(
            [packed, jnp.zeros((PACK_ROWS, latent - each), jnp.float32)], axis=1
        )
        out_ref[each:, :] = packed.astype(jnp.bfloat16)


def project_kernel(peers, *refs):
    state_refs, refs = refs[: peers - 1], refs[peers - 1 :]
    full_refs, refs = refs[:6], refs[6:]
    up_ref, proj_ref, keep_ref, send_ref, flat_ref = refs
    each = full_refs[0].shape[0]
    heads, _, width = up_ref.shape
    columns = keep_ref.shape[2]
    span = math.lcm(2 * columns, 128)
    blocks = proj_ref.shape[1] // span
    drafts = each // heads
    numers = [full_refs[0][...], full_refs[3][...]]
    tops = [full_refs[1][...], full_refs[4][...]]
    totals = [full_refs[2][...], full_refs[5][...]]
    for state in state_refs:
        lines = state[each:, :each].astype(jnp.float32)
        numers.append(state[:each, :].astype(jnp.float32))
        tops.append(as_column(lines[0:1] + lines[1:2] + lines[2:3]))
        totals.append(as_column(lines[3:4] + lines[4:5] + lines[5:6]))
    best = tops[0]
    for other in tops[1:]:
        best = jnp.maximum(best, other)
    numer = total = 0.0
    for part, top, count in zip(numers, tops, totals):
        factor = jnp.exp2(top - best)
        numer = numer + part * factor
        total = total + count * factor
    latent_out = (numer / total).astype(jnp.bfloat16)
    for head in range(heads):
        value = jnp.dot(
            latent_out[head * drafts : (head + 1) * drafts],
            up_ref[head],
            preferred_element_type=jnp.float32,
        )
        flat_ref[:, head * width : (head + 1) * width] = value.astype(jnp.bfloat16)
    flat = flat_ref[...]
    first_core = lax.rem(lax.axis_index("ctx"), 2) == 0
    for block in range(blocks):
        part = jnp.dot(
            flat,
            proj_ref[:, block * span : (block + 1) * span],
            preferred_element_type=jnp.float32,
        )
        for pair in range(span // (2 * columns)):
            halves = []
            for side in range(2):
                shift = (2 * pair + side) * columns
                moved = part if shift == 0 else pltpu.roll(part, span - shift, 1)
                halves.append(moved[:, :columns])
            spot = block * (span // (2 * columns)) + pair
            keep_ref[spot] = jnp.where(first_core, halves[0], halves[1])
            send_ref[spot] = jnp.where(first_core, halves[1], halves[0]).astype(jnp.bfloat16)


def pair_kernel(keep_ref, got_ref, stay_ref, send_ref):
    side = lax.rem(lax.div(lax.axis_index("ctx"), 2), 2)
    for spot in range(stay_ref.shape[0]):
        mine = 2 * spot + side
        yours = 2 * spot + 1 - side
        stay_ref[spot] = keep_ref[mine] + got_ref[mine].astype(jnp.float32)
        send_ref[spot] = (keep_ref[yours] + got_ref[yours].astype(jnp.float32)).astype(jnp.bfloat16)


def quad_kernel(stay_ref, got_ref, own_ref, *out_refs):
    outer = lax.div(lax.axis_index("ctx"), 4)

    def both(spot):
        return stay_ref[spot] + got_ref[spot].astype(jnp.float32)

    for peer, out_ref in enumerate(out_refs, 1):
        out_ref[...] = both(lax.bitwise_xor(outer, peer)).astype(jnp.bfloat16)
    own_ref[...] = both(outer)


def call(kernel, outs, values, specs=None, out_specs=None, scratch=(), limit=24):
    return pl.pallas_call(
        kernel,
        out_shape=outs,
        in_specs=specs or [pl.BlockSpec() for _ in values],
        out_specs=out_specs or [pl.BlockSpec() for _ in outs],
        scratch_shapes=list(scratch),
        compiler_params=pltpu.CompilerParams(vmem_limit_bytes=limit << 20),
    )(*values)


def shaped(*shape, dtype=jnp.float32):
    return jax.ShapeDtypeStruct(shape, dtype)


def on_device(count, queries, cache, draft_latent, lengths, parents, value_up, out_proj):
    drafts, heads_here, width = queries.shape[1:]
    latent = value_up.shape[1]
    block_len = cache.shape[1]
    inner = 4
    outer = count // inner
    chips = count // 2
    columns = out_proj.shape[1] // count
    each = heads_here * drafts
    bf16 = jnp.bfloat16
    myself = lax.axis_index("ctx")

    half = block_len // 2

    def bias_of(*spans):
        spots = [
            lax.bitwise_xor(myself, bit) * block_len + jnp.arange(low, high, dtype=jnp.int32)
            for bit, low, high in spans
        ]
        live = jnp.concatenate(spots)[None, :] < lengths[0]
        return jnp.where(live, 0.0, neg_fill).astype(jnp.float32)

    def swap(value, bits):
        return lax.ppermute(value, "ctx", [(i, i ^ bits) for i in range(count)])

    keys_own = jnp.transpose(cache[0])
    own_low, own_high = keys_own[:, :half], keys_own[:, half:]
    across_low = swap(own_low, 2)
    across_high = swap(own_high, 2)
    keys_core = swap(keys_own, 1)
    sent = {0: queries[0]}
    bit = outer // 2
    while bit:
        for peer in list(sent):
            sent[peer ^ bit] = swap(sent[peer], inner * bit)
        bit //= 2
    rows = [
        jnp.transpose(sent[peer], (1, 0, 2)).reshape(each, width) for peer in range(outer)
    ]
    own_rows = rows[0]
    far_low = swap(across_low, 1)
    far_high = swap(across_high, 1)

    state_shape = (shaped(outer * each, latent), shaped(outer * each, 1), shaped(outer * each, 1))
    own_shape = (shaped(each, latent), shaped(each, 1), shaped(each, 1))
    proj_here = jnp.where(lengths[0] > -1, out_proj, jnp.zeros_like(out_proj))
    *drafted, up_here = call(
        draft_kernel,
        own_shape + (shaped(*value_up.shape, dtype=bf16),),
        (own_rows, draft_latent[0], parents, value_up),
    )
    low, high = (0, half), (half, block_len)
    state = call(
        lambda *refs: first_kernel(outer, *refs),
        state_shape,
        (bias_of((0, *low), (0, *high), (1, 0, block_len)), *rows, own_low, own_high, keys_core),
    )
    state = call(
        lambda *refs: middle_kernel(outer, *refs),
        state_shape,
        (bias_of((2, *low), (3, *low)), *rows, across_low, far_low, *state),
    )
    state = call(
        lambda *refs: middle_kernel(outer, *refs),
        state_shape,
        (bias_of((2, *high)), *rows, across_high, *state),
    )
    done = call(
        lambda *refs: last_kernel(outer, *refs),
        own_shape
        + tuple(shaped(each + PACK_ROWS, latent, dtype=bf16) for _ in range(outer - 1)),
        (bias_of((3, *high)), *rows, far_high, *state),
    )
    whole, states = done[:3], done[3:]
    got = [swap(states[peer - 1], inner * peer) for peer in range(outer - 1, 0, -1)]
    keep, send = call(
        lambda *refs: project_kernel(outer, *refs),
        (shaped(chips, drafts, columns), shaped(chips, drafts, columns, dtype=bf16)),
        (*got, *whole, *drafted, up_here, proj_here),
        scratch=[pltpu.VMEM((drafts, heads_here * value_up.shape[2]), bf16)],
    )
    stay, send = call(
        pair_kernel,
        (shaped(chips // 2, drafts, columns), shaped(chips // 2, drafts, columns, dtype=bf16)),
        (keep, swap(send, 1)),
    )
    own, *parts = call(
        quad_kernel,
        (shaped(drafts, columns),)
        + tuple(shaped(drafts, columns, dtype=bf16) for _ in range(outer - 1)),
        (stay, swap(send, 2)),
    )
    result = own
    for peer in range(outer - 1, 0, -1):
        result = result + swap(parts[peer - 1], inner * peer).astype(jnp.float32)
    return result.astype(bf16)


def solution(mesh):
    in_specs = (
        P("grp", None, "ctx", None),
        P("grp", "ctx", None),
        P("grp", None, None),
        P("grp"),
        P("grp", None),
        P("ctx", None, None),
        P("ctx", None),
    )
    count = mesh.shape["ctx"]

    def body(*args):
        return on_device(count, *args)

    return jax.shard_map(
        body, mesh=mesh, in_specs=in_specs, out_specs=P("grp", "ctx"), check_vma=False
    )
```

```python
import math

import jax
import jax.numpy as jnp
from jax import lax
from jax.experimental import pallas as pl
from jax.experimental.pallas import tpu as pltpu
from jax.sharding import PartitionSpec as P


yarn_factor = 1.0 + 0.1 * math.log(32.0)
score_scale = yarn_factor * yarn_factor / math.sqrt(192.0)
log2_scale = score_scale / math.log(2.0)
neg_fill = -1e30
low_top = -1e29
PACK_ROWS = 8


NT = (((1,), (1,)), ((), ()))


def weights_of(masked, top):
    weights = jnp.exp2(masked - top).astype(jnp.bfloat16)
    return weights, jnp.sum(weights.astype(jnp.float32), axis=1, keepdims=True)


def as_row(column):
    count = column.shape[0]
    eye = lax.broadcasted_iota(jnp.int32, (count, count), 0) == lax.broadcasted_iota(
        jnp.int32, (count, count), 1
    )
    return jnp.sum(jnp.where(eye, column, 0.0), axis=0, keepdims=True)


def as_column(row):
    count = row.shape[1]
    eye = lax.broadcasted_iota(jnp.int32, (count, count), 0) == lax.broadcasted_iota(
        jnp.int32, (count, count), 1
    )
    return jnp.sum(jnp.where(eye, row, 0.0), axis=1, keepdims=True)


def tree_bias(parents):
    drafts = parents.shape[1]
    order = lax.broadcasted_iota(jnp.int32, (drafts, drafts), 1)
    self_order = lax.broadcasted_iota(jnp.int32, (drafts, drafts), 0)
    parent = as_column(parents.astype(jnp.float32)).astype(jnp.int32)
    reach = jnp.where((parent == order) | (self_order == order), 1.0, 0.0)
    covered = 1
    while covered < drafts:
        step = reach.astype(jnp.bfloat16)
        grown = jnp.dot(step, step, preferred_element_type=jnp.float32)
        reach = jnp.where(grown > 0.5, 1.0, 0.0)
        covered *= 2
    return jnp.where(reach > 0.5, 0.0, neg_fill)


def draft_kernel(
    q_ref, keys_ref, parents_ref, up_from, numer_ref, top_ref, total_ref, up_ref
):
    up_ref[...] = up_from[...]
    latent = numer_ref.shape[1]
    keys = keys_ref[...]
    repeats = q_ref.shape[0] // keys.shape[0]
    bias = jnp.concatenate([tree_bias(parents_ref[...])] * repeats, axis=0)
    scores = lax.dot_general(q_ref[...], keys, NT, preferred_element_type=jnp.float32)
    masked = scores * log2_scale + bias
    top = jnp.max(masked, axis=1, keepdims=True)
    weights, total = weights_of(masked, top)
    numer_ref[...] = jnp.dot(weights, keys[:, :latent], preferred_element_type=jnp.float32)
    top_ref[...] = top
    total_ref[...] = total


def fold(rows, key_refs, bias_ref, carry, latent):
    blocks, tops = [], []
    at = 0
    for key_ref in key_refs:
        scores = jnp.dot(rows, key_ref[...], preferred_element_type=jnp.float32)
        masked = scores * log2_scale + bias_ref[:, at : at + key_ref.shape[1]]
        at += key_ref.shape[1]
        blocks.append(masked)
        tops.append(jnp.max(masked, axis=1, keepdims=True))
    top = carry[1] if carry is not None else jnp.full_like(tops[0], low_top)
    for other in tops:
        top = jnp.maximum(top, other)
    numer = total = None
    if carry is not None:
        factor = jnp.exp2(carry[1] - top)
        numer, total = carry[0] * factor, carry[2] * factor
    for key_ref, masked in zip(key_refs, blocks):
        weights, count = weights_of(masked, top)
        part = lax.dot_general(weights, key_ref[:latent, :], NT, preferred_element_type=jnp.float32)
        numer = part if numer is None else numer + part
        total = count if total is None else total + count
    return numer, top, total


def join_rows(q_refs):
    return jnp.concatenate([q[...] for q in q_refs], axis=0)


def first_kernel(peers, bias_ref, *refs):
    q_refs, key_refs, out_refs = refs[:peers], refs[peers:-3], refs[-3:]
    state = fold(join_rows(q_refs), key_refs, bias_ref, None, out_refs[0].shape[1])
    for out_ref, value in zip(out_refs, state):
        out_ref[...] = value


def middle_kernel(peers, bias_ref, *refs):
    q_refs, (key_ref, *carry_refs), out_refs = refs[:peers], refs[peers:-3], refs[-3:]
    carry = tuple(join_rows(carry_refs[part::3]) for part in range(3))
    state = fold(join_rows(q_refs), [key_ref], bias_ref, carry, out_refs[0].shape[1])
    for out_ref, value in zip(out_refs, state):
        out_ref[...] = value


def pieces(row):
    high = row.astype(jnp.bfloat16).astype(jnp.float32)
    rest = row - high
    middle = rest.astype(jnp.bfloat16).astype(jnp.float32)
    return [high, middle, rest - middle]


def last_kernel(peers, bias_ref, *refs):
    q_refs, (key_ref, *rest) = refs[:peers], refs[peers:]
    numer_ref, top_ref, total_ref, own_refs, out_refs = *rest[:3], rest[3:6], rest[6:]
    carry = (numer_ref[...], top_ref[...], total_ref[...])
    latent = numer_ref.shape[1]
    numer, top, total = fold(join_rows(q_refs), [key_ref], bias_ref, carry, latent)
    each = q_refs[0].shape[0]
    for own_ref, value in zip(own_refs, (numer, top, total)):
        own_ref[...] = value[:each]
    for peer, out_ref in enumerate(out_refs, 1):
        here = slice(peer * each, (peer + 1) * each)
        out_ref[:each, :] = numer[here].astype(jnp.bfloat16)
        lines = pieces(as_row(top[here])) + pieces(as_row(total[here]))
        lines += [jnp.zeros_like(lines[0])] * (PACK_ROWS - len(lines))
        packed = jnp.concatenate(lines, axis=0)
        packed = jnp.concatenate(
            [packed, jnp.zeros((PACK_ROWS, latent - each), jnp.float32)], axis=1
        )
        out_ref[each:, :] = packed.astype(jnp.bfloat16)


def project_kernel(peers, *refs):
    state_refs, refs = refs[: peers - 1], refs[peers - 1 :]
    full_refs, refs = refs[:6], refs[6:]
    up_ref, proj_ref, keep_ref, send_ref, flat_ref = refs
    each = full_refs[0].shape[0]
    heads, _, width = up_ref.shape
    columns = keep_ref.shape[2]
    span = math.lcm(2 * columns, 128)
    blocks = proj_ref.shape[1] // span
    drafts = each // heads
    numers = [full_refs[0][...], full_refs[3][...]]
    tops = [full_refs[1][...], full_refs[4][...]]
    totals = [full_refs[2][...], full_refs[5][...]]
    for state in state_refs:
        lines = state[each:, :each].astype(jnp.float32)
        numers.append(state[:each, :].astype(jnp.float32))
        tops.append(as_column(lines[0:1] + lines[1:2] + lines[2:3]))
        totals.append(as_column(lines[3:4] + lines[4:5] + lines[5:6]))
    best = tops[0]
    for other in tops[1:]:
        best = jnp.maximum(best, other)
    numer = total = 0.0
    for part, top, count in zip(numers, tops, totals):
        factor = jnp.exp2(top - best)
        numer = numer + part * factor
        total = total + count * factor
    latent_out = (numer / total).astype(jnp.bfloat16)
    for head in range(heads):
        value = jnp.dot(
            latent_out[head * drafts : (head + 1) * drafts],
            up_ref[head],
            preferred_element_type=jnp.float32,
        )
        flat_ref[:, head * width : (head + 1) * width] = value.astype(jnp.bfloat16)
    flat = flat_ref[...]
    first_core = lax.rem(lax.axis_index("ctx"), 2) == 0
    for block in range(blocks):
        part = jnp.dot(
            flat,
            proj_ref[:, block * span : (block + 1) * span],
            preferred_element_type=jnp.float32,
        )
        for pair in range(span // (2 * columns)):
            halves = []
            for side in range(2):
                shift = (2 * pair + side) * columns
                moved = part if shift == 0 else pltpu.roll(part, span - shift, 1)
                halves.append(moved[:, :columns])
            spot = block * (span // (2 * columns)) + pair
            keep_ref[spot] = jnp.where(first_core, halves[0], halves[1])
            send_ref[spot] = jnp.where(first_core, halves[1], halves[0]).astype(jnp.bfloat16)


def pair_kernel(keep_ref, got_ref, stay_ref, send_ref):
    side = lax.rem(lax.div(lax.axis_index("ctx"), 2), 2)
    for spot in range(stay_ref.shape[0]):
        mine = 2 * spot + side
        yours = 2 * spot + 1 - side
        stay_ref[spot] = keep_ref[mine] + got_ref[mine].astype(jnp.float32)
        send_ref[spot] = (keep_ref[yours] + got_ref[yours].astype(jnp.float32)).astype(jnp.bfloat16)


def quad_kernel(stay_ref, got_ref, own_ref, *out_refs):
    outer = lax.div(lax.axis_index("ctx"), 4)

    def both(spot):
        return stay_ref[spot] + got_ref[spot].astype(jnp.float32)

    for peer, out_ref in enumerate(out_refs, 1):
        out_ref[...] = both(lax.bitwise_xor(outer, peer)).astype(jnp.bfloat16)
    own_ref[...] = both(outer)


def call(kernel, outs, values, specs=None, out_specs=None, scratch=(), limit=24):
    return pl.pallas_call(
        kernel,
        out_shape=outs,
        in_specs=specs or [pl.BlockSpec() for _ in values],
        out_specs=out_specs or [pl.BlockSpec() for _ in outs],
        scratch_shapes=list(scratch),
        compiler_params=pltpu.CompilerParams(vmem_limit_bytes=limit << 20),
    )(*values)


def shaped(*shape, dtype=jnp.float32):
    return jax.ShapeDtypeStruct(shape, dtype)


def on_device(count, queries, cache, draft_latent, lengths, parents, value_up, out_proj):
    drafts, heads_here, width = queries.shape[1:]
    latent = value_up.shape[1]
    block_len = cache.shape[1]
    inner = 4
    outer = count // inner
    chips = count // 2
    columns = out_proj.shape[1] // count
    each = heads_here * drafts
    bf16 = jnp.bfloat16
    myself = lax.axis_index("ctx")

    def bias_of(*bits):
        spots = [
            lax.bitwise_xor(myself, bit) * block_len + jnp.arange(block_len, dtype=jnp.int32)
            for bit in bits
        ]
        live = jnp.concatenate(spots)[None, :] < lengths[0]
        return jnp.where(live, 0.0, neg_fill).astype(jnp.float32)

    def swap(value, bits):
        return lax.ppermute(value, "ctx", [(i, i ^ bits) for i in range(count)])

    def on_chip(value):
        return jnp.where(lengths[0] > -1, value, jnp.zeros_like(value))

    keys_own = jnp.transpose(cache[0])
    keys_across = swap(keys_own, 2)
    keys_core = swap(keys_own, 1)
    keys_far = swap(keys_across, 1)
    sent = {0: queries[0]}
    bit = outer // 2
    while bit:
        for peer in list(sent):
            sent[peer ^ bit] = swap(sent[peer], inner * bit)
        bit //= 2
    peers = [*range(0, outer, 2), *range(1, outer, 2)]
    rows = [jnp.transpose(sent[peer], (1, 0, 2)).reshape(each, width) for peer in peers]
    own_rows = rows[0]

    def state_of(blocks):
        return tuple(shaped(blocks * each, size) for size in (latent, 1, 1))

    own_shape = state_of(1)
    proj_here = on_chip(out_proj)
    *drafted, up_here = call(
        draft_kernel,
        own_shape + (shaped(*value_up.shape, dtype=bf16),),
        (own_rows, draft_latent[0], parents, value_up),
    )
    keys_here = on_chip(keys_own)
    parts = []
    for some in (rows[: outer // 2], rows[outer // 2 :]):
        parts += call(
            lambda *refs: first_kernel(outer // 2, *refs),
            state_of(outer // 2),
            (bias_of(0, 1), *some, keys_here, keys_core),
        )
    state = call(
        lambda *refs: middle_kernel(outer, *refs),
        state_of(outer),
        (bias_of(2), *rows, keys_across, *parts),
    )
    done = call(
        lambda *refs: last_kernel(outer, *refs),
        own_shape
        + tuple(shaped(each + PACK_ROWS, latent, dtype=bf16) for _ in range(outer - 1)),
        (bias_of(3), *rows, keys_far, *state),
    )
    whole, states = done[:3], dict(zip(peers[1:], done[3:]))
    got = [swap(states[peer], inner * peer) for peer in range(outer - 1, 0, -1)]
    keep, send = call(
        lambda *refs: project_kernel(outer, *refs),
        (shaped(chips, drafts, columns), shaped(chips, drafts, columns, dtype=bf16)),
        (*got, *whole, *drafted, up_here, proj_here),
        scratch=[pltpu.VMEM((drafts, heads_here * value_up.shape[2]), bf16)],
    )
    stay, send = call(
        pair_kernel,
        (shaped(chips // 2, drafts, columns), shaped(chips // 2, drafts, columns, dtype=bf16)),
        (keep, swap(send, 1)),
    )
    own, *parts = call(
        quad_kernel,
        (shaped(drafts, columns),)
        + tuple(shaped(drafts, columns, dtype=bf16) for _ in range(outer - 1)),
        (stay, swap(send, 2)),
    )
    result = own
    for peer in range(outer - 1, 0, -1):
        result = result + swap(parts[peer - 1], inner * peer).astype(jnp.float32)
    return result.astype(bf16)


def solution(mesh):
    in_specs = (
        P("grp", None, "ctx", None),
        P("grp", "ctx", None),
        P("grp", None, None),
        P("grp"),
        P("grp", None),
        P("ctx", None, None),
        P("ctx", None),
    )
    count = mesh.shape["ctx"]

    def body(*args):
        return on_device(count, *args)

    return jax.shard_map(
        body, mesh=mesh, in_specs=in_specs, out_specs=P("grp", "ctx"), check_vma=False
    )
```

```python
import math

import jax
import jax.numpy as jnp
from jax import lax
from jax.experimental import pallas as pl
from jax.experimental.pallas import tpu as pltpu
from jax.sharding import PartitionSpec as P


yarn_factor = 1.0 + 0.1 * math.log(32.0)
score_scale = yarn_factor * yarn_factor / math.sqrt(192.0)
log2_scale = score_scale / math.log(2.0)
neg_fill = -1e30
low_top = -1e29
PACK_ROWS = 8


NT = (((1,), (1,)), ((), ()))


def weights_of(masked, top):
    weights = jnp.exp2(masked - top).astype(jnp.bfloat16)
    return weights, jnp.sum(weights.astype(jnp.float32), axis=1, keepdims=True)


def as_row(column):
    count = column.shape[0]
    eye = lax.broadcasted_iota(jnp.int32, (count, count), 0) == lax.broadcasted_iota(
        jnp.int32, (count, count), 1
    )
    return jnp.sum(jnp.where(eye, column, 0.0), axis=0, keepdims=True)


def as_column(row):
    count = row.shape[1]
    eye = lax.broadcasted_iota(jnp.int32, (count, count), 0) == lax.broadcasted_iota(
        jnp.int32, (count, count), 1
    )
    return jnp.sum(jnp.where(eye, row, 0.0), axis=1, keepdims=True)


def tree_bias(parents):
    drafts = parents.shape[1]
    order = lax.broadcasted_iota(jnp.int32, (drafts, drafts), 1)
    self_order = lax.broadcasted_iota(jnp.int32, (drafts, drafts), 0)
    parent = as_column(parents.astype(jnp.float32)).astype(jnp.int32)
    reach = jnp.where((parent == order) | (self_order == order), 1.0, 0.0)
    covered = 1
    while covered < drafts:
        step = reach.astype(jnp.bfloat16)
        grown = jnp.dot(step, step, preferred_element_type=jnp.float32)
        reach = jnp.where(grown > 0.5, 1.0, 0.0)
        covered *= 2
    return jnp.where(reach > 0.5, 0.0, neg_fill)


def merge(states):
    best = states[0][1]
    for state in states[1:]:
        best = jnp.maximum(best, state[1])
    numer = total = 0.0
    for part, top, count in states:
        factor = jnp.exp2(top - best)
        numer = numer + part * factor
        total = total + count * factor
    return numer, best, total


def draft_kernel(q_ref, keys_ref, parents_ref, up_from, *refs):
    own_refs, out_refs, up_ref = refs[:3], refs[3:6], refs[6]
    up_ref[...] = up_from[...]
    latent = own_refs[0].shape[1]
    keys = keys_ref[...]
    repeats = q_ref.shape[0] // keys.shape[0]
    bias = jnp.concatenate([tree_bias(parents_ref[...])] * repeats, axis=0)
    scores = lax.dot_general(q_ref[...], keys, NT, preferred_element_type=jnp.float32)
    masked = scores * log2_scale + bias
    top = jnp.max(masked, axis=1, keepdims=True)
    weights, total = weights_of(masked, top)
    numer = jnp.dot(weights, keys[:, :latent], preferred_element_type=jnp.float32)
    put(merge([(numer, top, total), tuple(ref[...] for ref in own_refs)]), out_refs)


def fold(rows, key_refs, bias_ref, carry, latent):
    blocks, tops = [], []
    at = 0
    for key_ref in key_refs:
        scores = jnp.dot(rows, key_ref[...], preferred_element_type=jnp.float32)
        masked = scores * log2_scale + bias_ref[:, at : at + key_ref.shape[1]]
        at += key_ref.shape[1]
        blocks.append(masked)
        tops.append(jnp.max(masked, axis=1, keepdims=True))
    top = carry[1] if carry is not None else jnp.full_like(tops[0], low_top)
    for other in tops:
        top = jnp.maximum(top, other)
    numer = total = None
    if carry is not None:
        factor = jnp.exp2(carry[1] - top)
        numer, total = carry[0] * factor, carry[2] * factor
    for key_ref, masked in zip(key_refs, blocks):
        weights, count = weights_of(masked, top)
        part = lax.dot_general(weights, key_ref[:latent, :], NT, preferred_element_type=jnp.float32)
        numer = part if numer is None else numer + part
        total = count if total is None else total + count
    return numer, top, total


def join_rows(q_refs):
    return jnp.concatenate([q[...] for q in q_refs], axis=0)


def put(state, refs):
    blocks = len(refs) // 3
    each = refs[0].shape[0]
    for block in range(blocks):
        for part in range(3):
            refs[3 * block + part][...] = state[part][block * each : (block + 1) * each]


def first_kernel(peers, bias_ref, *refs):
    q_refs, key_refs, out_refs = refs[:peers], refs[peers : -3 * peers], refs[-3 * peers :]
    put(fold(join_rows(q_refs), key_refs, bias_ref, None, out_refs[0].shape[1]), out_refs)


def carried(refs):
    return tuple(join_rows(refs[part::3]) for part in range(3))


def middle_kernel(peers, bias_ref, *refs):
    q_refs, (key_ref, *refs) = refs[:peers], refs[peers:]
    carry_refs, out_refs = refs[: 3 * peers], refs[3 * peers :]
    latent = out_refs[0].shape[1]
    put(fold(join_rows(q_refs), [key_ref], bias_ref, carried(carry_refs), latent), out_refs)


def pieces(row):
    high = row.astype(jnp.bfloat16).astype(jnp.float32)
    rest = row - high
    middle = rest.astype(jnp.bfloat16).astype(jnp.float32)
    return [high, middle, rest - middle]


def pack(numer, top, total, out_ref):
    each, latent = numer.shape
    lanes = out_ref.shape[1]
    for group in range(latent // lanes):
        strip = numer[:, group * lanes : (group + 1) * lanes]
        out_ref[group * each : (group + 1) * each, :] = strip.astype(jnp.bfloat16)
    lines = pieces(as_row(top)) + pieces(as_row(total))
    lines += [jnp.zeros_like(lines[0])] * (PACK_ROWS - len(lines))
    packed = jnp.concatenate(lines, axis=0)
    if lanes > each:
        packed = jnp.concatenate(
            [packed, jnp.zeros((PACK_ROWS, lanes - each), jnp.float32)], axis=1
        )
    out_ref[out_ref.shape[0] - PACK_ROWS :, :] = packed.astype(jnp.bfloat16)


def unpack(state_ref, each):
    bottom = state_ref.shape[0] - PACK_ROWS
    lines = state_ref[bottom:, :each].astype(jnp.float32)
    top = as_column(lines[0:1] + lines[1:2] + lines[2:3])
    total = as_column(lines[3:4] + lines[4:5] + lines[5:6])
    strips = [state_ref[at : at + each, :] for at in range(0, bottom, each)]
    return jnp.concatenate(strips, axis=1).astype(jnp.float32), top, total


def last_kernel(peers, plain, bias_ref, *refs):
    q_refs, (key_ref, *refs) = refs[:peers], refs[peers:]
    carry_refs, out_refs = refs[: 3 * peers], refs[3 * peers :]
    latent = carry_refs[0].shape[1]
    state = fold(join_rows(q_refs), [key_ref], bias_ref, carried(carry_refs), latent)
    each = q_refs[0].shape[0]
    if plain:
        put([value[:each] for value in state], out_refs[:3])
        out_refs = out_refs[3:]
    for peer, out_ref in enumerate(out_refs, 1 if plain else 0):
        pack(*(value[peer * each : (peer + 1) * each] for value in state), out_ref)


def values_of(peers, refs, flat_ref):
    state_refs, own_refs, up_ref = refs[: peers - 1], refs[peers - 1 : peers + 2], refs[peers + 2]
    each = own_refs[0].shape[0]
    heads, _, width = up_ref.shape
    drafts = each // heads
    states = [unpack(state, each) for state in state_refs]
    numer, _, total = merge([tuple(ref[...] for ref in own_refs)] + states)
    latent_out = (numer / total).astype(jnp.bfloat16)
    for head in range(heads):
        value = jnp.dot(
            latent_out[head * drafts : (head + 1) * drafts],
            up_ref[head],
            preferred_element_type=jnp.float32,
        )
        flat_ref[:, head * width : (head + 1) * width] = value.astype(jnp.bfloat16)


def share(part, pair, spot, keep_ref, send_ref):
    columns = keep_ref.shape[2]
    first_core = lax.rem(lax.axis_index("ctx"), 2) == 0
    halves = []
    for side in range(2):
        shift = (2 * pair + side) * columns
        moved = part if shift == 0 else pltpu.roll(part, part.shape[1] - shift, 1)
        halves.append(moved[:, :columns])
    keep_ref[spot] = jnp.where(first_core, halves[0], halves[1])
    send_ref[spot] = jnp.where(first_core, halves[1], halves[0]).astype(jnp.bfloat16)


def project_kernel(across, flat, proj_ref, keep_ref, send_ref):
    side = lax.rem(lax.div(lax.axis_index("ctx"), 2), 2)
    side = 1 - side if across else side
    span = 2 * keep_ref.shape[2]
    for spot in range(keep_ref.shape[0]):
        at = pl.multiple_of((2 * spot + side) * span, span)
        part = jnp.dot(flat, proj_ref[:, pl.ds(at, span)], preferred_element_type=jnp.float32)
        share(part, 0, spot, keep_ref, send_ref)


def leaving_kernel(peers, *refs):
    proj_ref, flat_ref, keep_ref, send_ref = refs[-4:]
    values_of(peers, refs, flat_ref)
    project_kernel(1, flat_ref[...], proj_ref, keep_ref, send_ref)


def staying_kernel(flat_ref, proj_ref, keep_ref, send_ref):
    project_kernel(0, flat_ref[...], proj_ref, keep_ref, send_ref)


def add_kernel(keep_ref, got_ref, out_ref):
    out_ref[...] = (keep_ref[...] + got_ref[...].astype(jnp.float32)).astype(out_ref.dtype)


def whole_kernel(peers, *refs):
    proj_ref, flat_ref, keep_ref, send_ref = refs[-4:]
    values_of(peers, refs, flat_ref)
    flat = flat_ref[...]
    columns = keep_ref.shape[2]
    span = math.lcm(2 * columns, 128)
    pairs = span // (2 * columns)
    for block in range(proj_ref.shape[1] // span):
        part = jnp.dot(
            flat,
            proj_ref[:, block * span : (block + 1) * span],
            preferred_element_type=jnp.float32,
        )
        for pair in range(pairs):
            share(part, pair, block * pairs + pair, keep_ref, send_ref)


def pair_kernel(keep_ref, got_ref, stay_ref, send_ref):
    side = lax.rem(lax.div(lax.axis_index("ctx"), 2), 2)
    for spot in range(stay_ref.shape[0]):
        mine = 2 * spot + side
        yours = 2 * spot + 1 - side
        stay_ref[spot] = keep_ref[mine] + got_ref[mine].astype(jnp.float32)
        send_ref[spot] = (keep_ref[yours] + got_ref[yours].astype(jnp.float32)).astype(jnp.bfloat16)


def quad_kernel(stay_ref, got_ref, own_ref, *out_refs):
    outer = lax.div(lax.axis_index("ctx"), 4)

    def both(spot):
        return stay_ref[spot] + got_ref[spot].astype(jnp.float32)

    for peer, out_ref in enumerate(out_refs, 1):
        out_ref[...] = both(lax.bitwise_xor(outer, peer)).astype(jnp.bfloat16)
    own_ref[...] = both(outer)


def call(kernel, outs, values, specs=None, out_specs=None, scratch=(), limit=24):
    return pl.pallas_call(
        kernel,
        out_shape=outs,
        in_specs=specs or [pl.BlockSpec() for _ in values],
        out_specs=out_specs or [pl.BlockSpec() for _ in outs],
        scratch_shapes=list(scratch),
        compiler_params=pltpu.CompilerParams(vmem_limit_bytes=limit << 20),
    )(*values)


def shaped(*shape, dtype=jnp.float32):
    return jax.ShapeDtypeStruct(shape, dtype)


def on_device(count, queries, cache, draft_latent, lengths, parents, value_up, out_proj):
    drafts, heads_here, width = queries.shape[1:]
    latent = value_up.shape[1]
    block_len = cache.shape[1]
    inner = 4
    outer = count // inner
    chips = count // 2
    columns = out_proj.shape[1] // count
    each = heads_here * drafts
    bf16 = jnp.bfloat16
    myself = lax.axis_index("ctx")

    def bias_of(*bits):
        spots = [
            lax.bitwise_xor(myself, bit) * block_len + jnp.arange(block_len, dtype=jnp.int32)
            for bit in bits
        ]
        live = jnp.concatenate(spots)[None, :] < lengths[0]
        return jnp.where(live, 0.0, neg_fill).astype(jnp.float32)

    def swap(value, bits):
        return lax.ppermute(value, "ctx", [(i, i ^ bits) for i in range(count)])

    def on_chip(value):
        return jnp.where(lengths[0] > -1, value, jnp.zeros_like(value))

    keys_own = jnp.transpose(cache[0])
    keys_across = swap(keys_own, 2)
    keys_core = swap(keys_own, 1)
    keys_far = swap(keys_across, 1)
    sent = {0: queries[0]}
    bit = outer // 2
    while bit:
        for peer in list(sent):
            sent[peer ^ bit] = swap(sent[peer], inner * bit)
        bit //= 2
    rows = {
        peer: jnp.transpose(value, (1, 0, 2)).reshape(each, width) for peer, value in sent.items()
    }
    own_rows = rows[0]
    everyone = list(range(outer))

    def pick(table, peers):
        return [table[peer] for peer in peers]

    def state_of(blocks):
        return tuple(shaped(each, size) for size in (latent, 1, 1)) * blocks

    own_shape = state_of(1)
    proj_here = on_chip(out_proj)
    keys_here = on_chip(keys_own)
    state = {}

    def save(peers, values):
        for spot, peer in enumerate(peers):
            state[peer] = list(values[3 * spot : 3 * spot + 3])

    for part in range(2):
        peers = everyone[part::2]
        values = call(
            lambda *refs: first_kernel(outer // 2, *refs),
            state_of(outer // 2),
            (bias_of(0, 1), *pick(rows, peers), keys_here, keys_core),
        )
        save(peers, values)
    values = call(
        lambda *refs: middle_kernel(outer, *refs),
        state_of(outer),
        (bias_of(2), *pick(rows, everyone), keys_across, *sum(pick(state, everyone), [])),
    )
    save(everyone, values)
    lanes = math.gcd(latent, 128)
    packed = shaped(each * latent // lanes + PACK_ROWS, lanes, dtype=bf16)
    got = []
    for near in (False, True):
        peers = everyone[: outer // 2] if near else everyone[outer // 2 :]
        values = call(
            lambda *refs, near=near: last_kernel(outer // 2, near, *refs),
            (own_shape if near else ()) + (packed,) * (len(peers) - near),
            (bias_of(3), *pick(rows, peers), keys_far, *sum(pick(state, peers), [])),
        )
        if near:
            whole, values, peers = values[:3], values[3:], peers[1:]
        got += [swap(value, inner * peer) for peer, value in zip(peers, values)]
    proj_here = on_chip(out_proj)
    *whole, up_here = call(
        draft_kernel,
        own_shape + (shaped(*value_up.shape, dtype=bf16),),
        (own_rows, draft_latent[0], parents, value_up, *whole),
    )
    inputs = (*got, *whole, up_here, proj_here)
    flat_shape = shaped(drafts, heads_here * value_up.shape[2], dtype=bf16)

    def halves_of(chips):
        return shaped(chips, drafts, columns), shaped(chips, drafts, columns, dtype=bf16)

    if 2 * columns % 128 == 0:
        flat, keep, send = call(
            lambda *refs: leaving_kernel(outer, *refs), (flat_shape, *halves_of(chips // 2)), inputs
        )
        got_leaving = swap(send, 1)
        stay, stay_send = call(staying_kernel, halves_of(chips // 2), (flat, proj_here))
        send = call(add_kernel, (halves_of(chips // 2)[1],), (keep, got_leaving))[0]
        got_staying = swap(stay_send, 1)
        stay = call(add_kernel, (halves_of(chips // 2)[0],), (stay, got_staying))[0]
    else:
        flat, keep, send = call(
            lambda *refs: whole_kernel(outer, *refs), (flat_shape, *halves_of(chips)), inputs
        )
        stay, send = call(pair_kernel, halves_of(chips // 2), (keep, swap(send, 1)))
    own, *parts = call(
        quad_kernel,
        (shaped(drafts, columns),)
        + tuple(shaped(drafts, columns, dtype=bf16) for _ in range(outer - 1)),
        (stay, swap(send, 2)),
    )
    result = own
    for peer in range(outer - 1, 0, -1):
        result = result + swap(parts[peer - 1], inner * peer).astype(jnp.float32)
    return result.astype(bf16)


def solution(mesh):
    in_specs = (
        P("grp", None, "ctx", None),
        P("grp", "ctx", None),
        P("grp", None, None),
        P("grp"),
        P("grp", None),
        P("ctx", None, None),
        P("ctx", None),
    )
    count = mesh.shape["ctx"]

    def body(*args):
        return on_device(count, *args)

    return jax.shard_map(
        body, mesh=mesh, in_specs=in_specs, out_specs=P("grp", "ctx"), check_vma=False
    )
```

```python
import math

import jax
import jax.numpy as jnp
from jax import lax
from jax.experimental import pallas as pl
from jax.experimental.pallas import tpu as pltpu
from jax.sharding import PartitionSpec as P


yarn_factor = 1.0 + 0.1 * math.log(32.0)
score_scale = yarn_factor * yarn_factor / math.sqrt(192.0)
log2_scale = score_scale / math.log(2.0)
neg_fill = -1e30
low_top = -1e29
PACK_ROWS = 8


NT = (((1,), (1,)), ((), ()))


def weights_of(masked, top):
    weights = jnp.exp2(masked - top).astype(jnp.bfloat16)
    return weights, jnp.sum(weights.astype(jnp.float32), axis=1, keepdims=True)


def as_row(column):
    count = column.shape[0]
    eye = lax.broadcasted_iota(jnp.int32, (count, count), 0) == lax.broadcasted_iota(
        jnp.int32, (count, count), 1
    )
    return jnp.sum(jnp.where(eye, column, 0.0), axis=0, keepdims=True)


def as_column(row):
    count = row.shape[1]
    eye = lax.broadcasted_iota(jnp.int32, (count, count), 0) == lax.broadcasted_iota(
        jnp.int32, (count, count), 1
    )
    return jnp.sum(jnp.where(eye, row, 0.0), axis=1, keepdims=True)


def tree_bias(parents):
    drafts = parents.shape[1]
    order = lax.broadcasted_iota(jnp.int32, (drafts, drafts), 1)
    self_order = lax.broadcasted_iota(jnp.int32, (drafts, drafts), 0)
    parent = as_column(parents.astype(jnp.float32)).astype(jnp.int32)
    reach = jnp.where((parent == order) | (self_order == order), 1.0, 0.0)
    covered = 1
    while covered < drafts:
        step = reach.astype(jnp.bfloat16)
        grown = jnp.dot(step, step, preferred_element_type=jnp.float32)
        reach = jnp.where(grown > 0.5, 1.0, 0.0)
        covered *= 2
    return jnp.where(reach > 0.5, 0.0, neg_fill)


def merge(states):
    best = states[0][1]
    for state in states[1:]:
        best = jnp.maximum(best, state[1])
    numer = total = 0.0
    for part, top, count in states:
        factor = jnp.exp2(top - best)
        numer = numer + part * factor
        total = total + count * factor
    return numer, best, total


def draft_kernel(q_ref, keys_ref, parents_ref, up_from, *refs):
    own_refs, out_refs, up_ref = refs[:3], refs[3:6], refs[6]
    up_ref[...] = up_from[...]
    latent = own_refs[0].shape[1]
    keys = keys_ref[...]
    repeats = q_ref.shape[0] // keys.shape[0]
    bias = jnp.concatenate([tree_bias(parents_ref[...])] * repeats, axis=0)
    scores = lax.dot_general(q_ref[...], keys, NT, preferred_element_type=jnp.float32)
    masked = scores * log2_scale + bias
    top = jnp.max(masked, axis=1, keepdims=True)
    weights, total = weights_of(masked, top)
    numer = jnp.dot(weights, keys[:, :latent], preferred_element_type=jnp.float32)
    put(merge([(numer, top, total), tuple(ref[...] for ref in own_refs)]), out_refs)


def fold(rows, key_refs, bias_ref, carry, latent):
    blocks, tops = [], []
    at = 0
    for key_ref in key_refs:
        scores = jnp.dot(rows, key_ref[...], preferred_element_type=jnp.float32)
        masked = scores * log2_scale + bias_ref[:, at : at + key_ref.shape[1]]
        at += key_ref.shape[1]
        blocks.append(masked)
        tops.append(jnp.max(masked, axis=1, keepdims=True))
    top = carry[1] if carry is not None else jnp.full_like(tops[0], low_top)
    for other in tops:
        top = jnp.maximum(top, other)
    numer = total = None
    if carry is not None:
        factor = jnp.exp2(carry[1] - top)
        numer, total = carry[0] * factor, carry[2] * factor
    for key_ref, masked in zip(key_refs, blocks):
        weights, count = weights_of(masked, top)
        part = lax.dot_general(weights, key_ref[:latent, :], NT, preferred_element_type=jnp.float32)
        numer = part if numer is None else numer + part
        total = count if total is None else total + count
    return numer, top, total


def join_rows(q_refs):
    return jnp.concatenate([q[...] for q in q_refs], axis=0)


def put(state, refs):
    blocks = len(refs) // 3
    each = refs[0].shape[0]
    for block in range(blocks):
        for part in range(3):
            refs[3 * block + part][...] = state[part][block * each : (block + 1) * each]


def first_kernel(peers, bias_ref, *refs):
    q_refs, key_refs, out_refs = refs[:peers], refs[peers : -3 * peers], refs[-3 * peers :]
    put(fold(join_rows(q_refs), key_refs, bias_ref, None, out_refs[0].shape[1]), out_refs)


def carried(refs):
    return tuple(join_rows(refs[part::3]) for part in range(3))


def middle_kernel(peers, bias_ref, *refs):
    q_refs, (key_ref, *refs) = refs[:peers], refs[peers:]
    carry_refs, out_refs = refs[: 3 * peers], refs[3 * peers :]
    latent = out_refs[0].shape[1]
    put(fold(join_rows(q_refs), [key_ref], bias_ref, carried(carry_refs), latent), out_refs)


def pieces(row):
    high = row.astype(jnp.bfloat16).astype(jnp.float32)
    rest = row - high
    middle = rest.astype(jnp.bfloat16).astype(jnp.float32)
    return [high, middle, rest - middle]


def pack(numer, top, total, out_ref):
    each, latent = numer.shape
    lanes = out_ref.shape[1]
    for group in range(latent // lanes):
        strip = numer[:, group * lanes : (group + 1) * lanes]
        out_ref[group * each : (group + 1) * each, :] = strip.astype(jnp.bfloat16)
    lines = pieces(as_row(top)) + pieces(as_row(total))
    lines += [jnp.zeros_like(lines[0])] * (PACK_ROWS - len(lines))
    packed = jnp.concatenate(lines, axis=0)
    if lanes > each:
        packed = jnp.concatenate(
            [packed, jnp.zeros((PACK_ROWS, lanes - each), jnp.float32)], axis=1
        )
    out_ref[out_ref.shape[0] - PACK_ROWS :, :] = packed.astype(jnp.bfloat16)


def unpack(state_ref, each):
    bottom = state_ref.shape[0] - PACK_ROWS
    lines = state_ref[bottom:, :each].astype(jnp.float32)
    top = as_column(lines[0:1] + lines[1:2] + lines[2:3])
    total = as_column(lines[3:4] + lines[4:5] + lines[5:6])
    strips = [state_ref[at : at + each, :] for at in range(0, bottom, each)]
    return jnp.concatenate(strips, axis=1).astype(jnp.float32), top, total


def last_kernel(peers, plain, bias_ref, *refs):
    q_refs, (key_ref, *refs) = refs[:peers], refs[peers:]
    carry_refs, out_refs = refs[: 3 * peers], refs[3 * peers :]
    latent = carry_refs[0].shape[1]
    state = fold(join_rows(q_refs), [key_ref], bias_ref, carried(carry_refs), latent)
    each = q_refs[0].shape[0]
    if plain:
        put([value[:each] for value in state], out_refs[:3])
        out_refs = out_refs[3:]
    for peer, out_ref in enumerate(out_refs, 1 if plain else 0):
        pack(*(value[peer * each : (peer + 1) * each] for value in state), out_ref)


def values_of(peers, refs, flat_ref):
    state_refs, own_refs, up_ref = refs[: peers - 1], refs[peers - 1 : peers + 2], refs[peers + 2]
    each = own_refs[0].shape[0]
    heads, _, width = up_ref.shape
    drafts = each // heads
    states = [unpack(state, each) for state in state_refs]
    numer, _, total = merge([tuple(ref[...] for ref in own_refs)] + states)
    latent_out = (numer / total).astype(jnp.bfloat16)
    for head in range(heads):
        value = jnp.dot(
            latent_out[head * drafts : (head + 1) * drafts],
            up_ref[head],
            preferred_element_type=jnp.float32,
        )
        flat_ref[:, head * width : (head + 1) * width] = value.astype(jnp.bfloat16)


def share(part, pair, spot, keep_ref, send_ref, cross=0):
    columns = keep_ref.shape[2]
    first_core = lax.rem(lax.axis_index("ctx") + cross, 2) == 0
    halves = []
    for side in range(2):
        shift = (2 * pair + side) * columns
        moved = part if shift == 0 else pltpu.roll(part, part.shape[1] - shift, 1)
        halves.append(moved[:, :columns])
    keep_ref[spot] = jnp.where(first_core, halves[0], halves[1])
    send_ref[spot] = jnp.where(first_core, halves[1], halves[0]).astype(jnp.bfloat16)


def project_kernel(across, flat, proj_ref, keep_ref, send_ref):
    side = lax.rem(lax.div(lax.axis_index("ctx"), 2), 2)
    side = 1 - side if across else side
    outer = lax.div(lax.axis_index("ctx"), 4)
    span = 2 * keep_ref.shape[2]
    for spot in range(keep_ref.shape[0]):
        at = pl.multiple_of((2 * spot + side) * span, span)
        part = jnp.dot(flat, proj_ref[:, pl.ds(at, span)], preferred_element_type=jnp.float32)
        elsewhere = jnp.where(outer == spot, 0, 1)
        share(part, 0, spot, keep_ref, send_ref, elsewhere + across)


def leaving_kernel(peers, *refs):
    proj_ref, flat_ref, keep_ref, send_ref = refs[-4:]
    values_of(peers, refs, flat_ref)
    project_kernel(1, flat_ref[...], proj_ref, keep_ref, send_ref)


def staying_kernel(flat_ref, proj_ref, keep_ref, send_ref):
    project_kernel(0, flat_ref[...], proj_ref, keep_ref, send_ref)


def add_kernel(keep_ref, got_ref, out_ref):
    out_ref[...] = (keep_ref[...] + got_ref[...].astype(jnp.float32)).astype(out_ref.dtype)


def whole_kernel(peers, *refs):
    proj_ref, flat_ref, keep_ref, send_ref = refs[-4:]
    values_of(peers, refs, flat_ref)
    flat = flat_ref[...]
    columns = keep_ref.shape[2]
    span = math.lcm(2 * columns, 128)
    pairs = span // (2 * columns)
    for block in range(proj_ref.shape[1] // span):
        part = jnp.dot(
            flat,
            proj_ref[:, block * span : (block + 1) * span],
            preferred_element_type=jnp.float32,
        )
        for pair in range(pairs):
            share(part, pair, block * pairs + pair, keep_ref, send_ref)


def pair_kernel(keep_ref, got_ref, stay_ref, send_ref):
    side = lax.rem(lax.div(lax.axis_index("ctx"), 2), 2)
    for spot in range(stay_ref.shape[0]):
        mine = 2 * spot + side
        yours = 2 * spot + 1 - side
        stay_ref[spot] = keep_ref[mine] + got_ref[mine].astype(jnp.float32)
        send_ref[spot] = (keep_ref[yours] + got_ref[yours].astype(jnp.float32)).astype(jnp.bfloat16)


def quad_kernel(stay_ref, got_ref, own_ref, *out_refs):
    outer = lax.div(lax.axis_index("ctx"), 4)

    def both(spot):
        return stay_ref[spot] + got_ref[spot].astype(jnp.float32)

    for peer, out_ref in enumerate(out_refs, 1):
        out_ref[...] = both(lax.bitwise_xor(outer, peer)).astype(jnp.bfloat16)
    own_ref[...] = both(outer)


def call(kernel, outs, values, specs=None, out_specs=None, scratch=(), limit=24):
    return pl.pallas_call(
        kernel,
        out_shape=outs,
        in_specs=specs or [pl.BlockSpec() for _ in values],
        out_specs=out_specs or [pl.BlockSpec() for _ in outs],
        scratch_shapes=list(scratch),
        compiler_params=pltpu.CompilerParams(vmem_limit_bytes=limit << 20),
    )(*values)


def shaped(*shape, dtype=jnp.float32):
    return jax.ShapeDtypeStruct(shape, dtype)


def on_device(count, queries, cache, draft_latent, lengths, parents, value_up, out_proj):
    drafts, heads_here, width = queries.shape[1:]
    latent = value_up.shape[1]
    block_len = cache.shape[1]
    inner = 4
    outer = count // inner
    chips = count // 2
    columns = out_proj.shape[1] // count
    each = heads_here * drafts
    bf16 = jnp.bfloat16
    myself = lax.axis_index("ctx")

    def bias_of(*bits):
        spots = [
            lax.bitwise_xor(myself, bit) * block_len + jnp.arange(block_len, dtype=jnp.int32)
            for bit in bits
        ]
        live = jnp.concatenate(spots)[None, :] < lengths[0]
        return jnp.where(live, 0.0, neg_fill).astype(jnp.float32)

    def swap(value, bits):
        return lax.ppermute(value, "ctx", [(i, i ^ bits) for i in range(count)])

    def on_chip(value):
        return jnp.where(lengths[0] > -1, value, jnp.zeros_like(value))

    keys_own = jnp.transpose(cache[0])
    keys_across = swap(keys_own, 3)
    keys_core = swap(keys_own, 1)
    keys_far = swap(keys_across, 1)
    sent = {0: queries[0]}
    bit = outer // 2
    while bit:
        for peer in list(sent):
            cross = 0 if peer else 1
            sent[peer ^ bit] = swap(sent[peer], inner * bit + cross)
        bit //= 2
    rows = {
        peer: jnp.transpose(value, (1, 0, 2)).reshape(each, width) for peer, value in sent.items()
    }
    own_rows = rows[0]
    everyone = list(range(outer))

    def pick(table, peers):
        return [table[peer] for peer in peers]

    def state_of(blocks):
        return tuple(shaped(each, size) for size in (latent, 1, 1)) * blocks

    own_shape = state_of(1)
    proj_here = on_chip(out_proj)
    keys_here = on_chip(keys_own)
    state = {}

    def save(peers, values):
        for spot, peer in enumerate(peers):
            state[peer] = list(values[3 * spot : 3 * spot + 3])

    for part in range(2):
        peers = everyone[part::2]
        values = call(
            lambda *refs: first_kernel(outer // 2, *refs),
            state_of(outer // 2),
            (bias_of(0, 1), *pick(rows, peers), keys_here, keys_core),
        )
        save(peers, values)
    values = call(
        lambda *refs: middle_kernel(outer, *refs),
        state_of(outer),
        (bias_of(3), *pick(rows, everyone), keys_across, *sum(pick(state, everyone), [])),
    )
    save(everyone, values)
    lanes = math.gcd(latent, 128)
    packed = shaped(each * latent // lanes + PACK_ROWS, lanes, dtype=bf16)
    got = []
    for near in (False, True):
        peers = everyone[: outer // 2] if near else everyone[outer // 2 :]
        values = call(
            lambda *refs, near=near: last_kernel(outer // 2, near, *refs),
            (own_shape if near else ()) + (packed,) * (len(peers) - near),
            (bias_of(2), *pick(rows, peers), keys_far, *sum(pick(state, peers), [])),
        )
        if near:
            whole, values, peers = values[:3], values[3:], peers[1:]
        got += [swap(value, inner * peer + 1) for peer, value in zip(peers, values)]
    proj_here = on_chip(out_proj)
    *whole, up_here = call(
        draft_kernel,
        own_shape + (shaped(*value_up.shape, dtype=bf16),),
        (own_rows, draft_latent[0], parents, value_up, *whole),
    )
    inputs = (*got, *whole, up_here, proj_here)
    flat_shape = shaped(drafts, heads_here * value_up.shape[2], dtype=bf16)

    def halves_of(chips):
        return shaped(chips, drafts, columns), shaped(chips, drafts, columns, dtype=bf16)

    cross = int(2 * columns % 128 == 0)
    if cross:
        flat, keep, send = call(
            lambda *refs: leaving_kernel(outer, *refs), (flat_shape, *halves_of(chips // 2)), inputs
        )
        got_leaving = swap(send, 1)
        stay, stay_send = call(staying_kernel, halves_of(chips // 2), (flat, proj_here))
        send = call(add_kernel, (halves_of(chips // 2)[1],), (keep, got_leaving))[0]
        got_staying = swap(stay_send, 1)
        stay = call(add_kernel, (halves_of(chips // 2)[0],), (stay, got_staying))[0]
    else:
        flat, keep, send = call(
            lambda *refs: whole_kernel(outer, *refs), (flat_shape, *halves_of(chips)), inputs
        )
        stay, send = call(pair_kernel, halves_of(chips // 2), (keep, swap(send, 1)))
    own, *parts = call(
        quad_kernel,
        (shaped(drafts, columns),)
        + tuple(shaped(drafts, columns, dtype=bf16) for _ in range(outer - 1)),
        (stay, swap(send, 2 + cross)),
    )
    result = own
    for peer in range(outer - 1, 0, -1):
        result = result + swap(parts[peer - 1], inner * peer + cross).astype(jnp.float32)
    return result.astype(bf16)


def solution(mesh):
    in_specs = (
        P("grp", None, "ctx", None),
        P("grp", "ctx", None),
        P("grp", None, None),
        P("grp"),
        P("grp", None),
        P("ctx", None, None),
        P("ctx", None),
    )
    count = mesh.shape["ctx"]

    def body(*args):
        return on_device(count, *args)

    return jax.shard_map(
        body, mesh=mesh, in_specs=in_specs, out_specs=P("grp", "ctx"), check_vma=False
    )
```

```python
import math

import jax
import jax.numpy as jnp
from jax import lax
from jax.experimental import pallas as pl
from jax.experimental.pallas import tpu as pltpu
from jax.sharding import PartitionSpec as P


yarn_factor = 1.0 + 0.1 * math.log(32.0)
score_scale = yarn_factor * yarn_factor / math.sqrt(192.0)
log2_scale = score_scale / math.log(2.0)
neg_fill = -1e30
low_top = -1e29
PACK_ROWS = 8


NT = (((1,), (1,)), ((), ()))


def weights_of(masked, top):
    weights = jnp.exp2(masked - top).astype(jnp.bfloat16)
    return weights, jnp.sum(weights.astype(jnp.float32), axis=1, keepdims=True)


def as_row(column):
    count = column.shape[0]
    eye = lax.broadcasted_iota(jnp.int32, (count, count), 0) == lax.broadcasted_iota(
        jnp.int32, (count, count), 1
    )
    return jnp.sum(jnp.where(eye, column, 0.0), axis=0, keepdims=True)


def as_column(row):
    count = row.shape[1]
    eye = lax.broadcasted_iota(jnp.int32, (count, count), 0) == lax.broadcasted_iota(
        jnp.int32, (count, count), 1
    )
    return jnp.sum(jnp.where(eye, row, 0.0), axis=1, keepdims=True)


def tree_bias(parents):
    drafts = parents.shape[1]
    order = lax.broadcasted_iota(jnp.int32, (drafts, drafts), 1)
    self_order = lax.broadcasted_iota(jnp.int32, (drafts, drafts), 0)
    parent = as_column(parents.astype(jnp.float32)).astype(jnp.int32)
    reach = jnp.where((parent == order) | (self_order == order), 1.0, 0.0)
    covered = 1
    while covered < drafts:
        step = reach.astype(jnp.bfloat16)
        grown = jnp.dot(step, step, preferred_element_type=jnp.float32)
        reach = jnp.where(grown > 0.5, 1.0, 0.0)
        covered *= 2
    return jnp.where(reach > 0.5, 0.0, neg_fill)


def merge(states):
    best = states[0][1]
    for state in states[1:]:
        best = jnp.maximum(best, state[1])
    numer = total = 0.0
    for part, top, count in states:
        factor = jnp.exp2(top - best)
        numer = numer + part * factor
        total = total + count * factor
    return numer, best, total


def draft_kernel(q_ref, keys_ref, parents_ref, up_from, *refs):
    own_refs, out_refs, up_ref = refs[:3], refs[3:6], refs[6]
    up_ref[...] = up_from[...]
    latent = own_refs[0].shape[1]
    keys = keys_ref[...]
    repeats = q_ref.shape[0] // keys.shape[0]
    bias = jnp.concatenate([tree_bias(parents_ref[...])] * repeats, axis=0)
    scores = lax.dot_general(q_ref[...], keys, NT, preferred_element_type=jnp.float32)
    masked = scores * log2_scale + bias
    top = jnp.max(masked, axis=1, keepdims=True)
    weights, total = weights_of(masked, top)
    numer = jnp.dot(weights, keys[:, :latent], preferred_element_type=jnp.float32)
    put(merge([(numer, top, total), tuple(ref[...] for ref in own_refs)]), out_refs)


def fold(rows, key_refs, bias_ref, carry, latent):
    blocks, tops = [], []
    at = 0
    for key_ref in key_refs:
        scores = jnp.dot(rows, key_ref[...], preferred_element_type=jnp.float32)
        masked = scores * log2_scale + bias_ref[:, at : at + key_ref.shape[1]]
        at += key_ref.shape[1]
        blocks.append(masked)
        tops.append(jnp.max(masked, axis=1, keepdims=True))
    top = carry[1] if carry is not None else jnp.full_like(tops[0], low_top)
    for other in tops:
        top = jnp.maximum(top, other)
    numer = total = None
    if carry is not None:
        factor = jnp.exp2(carry[1] - top)
        numer, total = carry[0] * factor, carry[2] * factor
    for key_ref, masked in zip(key_refs, blocks):
        weights, count = weights_of(masked, top)
        part = lax.dot_general(weights, key_ref[:latent, :], NT, preferred_element_type=jnp.float32)
        numer = part if numer is None else numer + part
        total = count if total is None else total + count
    return numer, top, total


def join_rows(q_refs):
    return jnp.concatenate([q[...] for q in q_refs], axis=0)


def put(state, refs):
    blocks = len(refs) // 3
    each = refs[0].shape[0]
    for block in range(blocks):
        for part in range(3):
            refs[3 * block + part][...] = state[part][block * each : (block + 1) * each]


def first_kernel(peers, bias_ref, *refs):
    q_refs, key_refs, out_refs = refs[:peers], refs[peers : -3 * peers], refs[-3 * peers :]
    put(fold(join_rows(q_refs), key_refs, bias_ref, None, out_refs[0].shape[1]), out_refs)


def carried(refs):
    return tuple(join_rows(refs[part::3]) for part in range(3))


def middle_kernel(peers, bias_ref, *refs):
    q_refs, (key_ref, *refs) = refs[:peers], refs[peers:]
    carry_refs, out_refs = refs[: 3 * peers], refs[3 * peers :]
    latent = out_refs[0].shape[1]
    put(fold(join_rows(q_refs), [key_ref], bias_ref, carried(carry_refs), latent), out_refs)


def pieces(row):
    high = row.astype(jnp.bfloat16).astype(jnp.float32)
    rest = row - high
    middle = rest.astype(jnp.bfloat16).astype(jnp.float32)
    return [high, middle, rest - middle]


def pack(numer, top, total, out_ref):
    each, latent = numer.shape
    lanes = out_ref.shape[1]
    for group in range(latent // lanes):
        strip = numer[:, group * lanes : (group + 1) * lanes]
        out_ref[group * each : (group + 1) * each, :] = strip.astype(jnp.bfloat16)
    lines = pieces(as_row(top)) + pieces(as_row(total))
    lines += [jnp.zeros_like(lines[0])] * (PACK_ROWS - len(lines))
    packed = jnp.concatenate(lines, axis=0)
    if lanes > each:
        packed = jnp.concatenate(
            [packed, jnp.zeros((PACK_ROWS, lanes - each), jnp.float32)], axis=1
        )
    out_ref[out_ref.shape[0] - PACK_ROWS :, :] = packed.astype(jnp.bfloat16)


def unpack(state_ref, each):
    bottom = state_ref.shape[0] - PACK_ROWS
    lines = state_ref[bottom:, :each].astype(jnp.float32)
    top = as_column(lines[0:1] + lines[1:2] + lines[2:3])
    total = as_column(lines[3:4] + lines[4:5] + lines[5:6])
    strips = [state_ref[at : at + each, :] for at in range(0, bottom, each)]
    return jnp.concatenate(strips, axis=1).astype(jnp.float32), top, total


def last_kernel(peers, plain, bias_ref, *refs):
    q_refs, (key_ref, *refs) = refs[:peers], refs[peers:]
    carry_refs, out_refs = refs[: 3 * peers], refs[3 * peers :]
    latent = carry_refs[0].shape[1]
    state = fold(join_rows(q_refs), [key_ref], bias_ref, carried(carry_refs), latent)
    each = q_refs[0].shape[0]
    if plain:
        put([value[:each] for value in state], out_refs[:3])
        out_refs = out_refs[3:]
    for peer, out_ref in enumerate(out_refs, 1 if plain else 0):
        pack(*(value[peer * each : (peer + 1) * each] for value in state), out_ref)


def values_of(peers, refs, flat_ref):
    state_refs, own_refs, up_ref = refs[: peers - 1], refs[peers - 1 : peers + 2], refs[peers + 2]
    each = own_refs[0].shape[0]
    heads, _, width = up_ref.shape
    drafts = each // heads
    states = [unpack(state, each) for state in state_refs]
    numer, _, total = merge([tuple(ref[...] for ref in own_refs)] + states)
    latent_out = (numer / total).astype(jnp.bfloat16)
    for head in range(heads):
        value = jnp.dot(
            latent_out[head * drafts : (head + 1) * drafts],
            up_ref[head],
            preferred_element_type=jnp.float32,
        )
        flat_ref[:, head * width : (head + 1) * width] = value.astype(jnp.bfloat16)


def share(part, pair, spot, keep_ref, send_ref, cross=0):
    columns = keep_ref.shape[2]
    first_core = lax.rem(lax.axis_index("ctx") + cross, 2) == 0
    halves = []
    for side in range(2):
        shift = (2 * pair + side) * columns
        moved = part if shift == 0 else pltpu.roll(part, part.shape[1] - shift, 1)
        halves.append(moved[:, :columns])
    keep_ref[spot] = jnp.where(first_core, halves[0], halves[1])
    send_ref[spot] = jnp.where(first_core, halves[1], halves[0]).astype(jnp.bfloat16)


def project_kernel(across, flat, proj_ref, keep_ref, send_ref):
    side = lax.rem(lax.div(lax.axis_index("ctx"), 2), 2)
    side = 1 - side if across else side
    outer = lax.div(lax.axis_index("ctx"), 4)
    span = 2 * keep_ref.shape[2]
    for spot in range(keep_ref.shape[0]):
        at = pl.multiple_of((2 * spot + side) * span, span)
        part = jnp.dot(flat, proj_ref[:, pl.ds(at, span)], preferred_element_type=jnp.float32)
        elsewhere = jnp.where(outer == spot, 0, 1)
        share(part, 0, spot, keep_ref, send_ref, elsewhere + across)


def leaving_kernel(peers, *refs):
    proj_ref, flat_ref, keep_ref, send_ref = refs[-4:]
    values_of(peers, refs, flat_ref)
    project_kernel(1, flat_ref[...], proj_ref, keep_ref, send_ref)


def staying_kernel(flat_ref, proj_ref, keep_ref, send_ref):
    project_kernel(0, flat_ref[...], proj_ref, keep_ref, send_ref)


def add_kernel(keep_ref, got_ref, out_ref):
    out_ref[...] = (keep_ref[...] + got_ref[...].astype(jnp.float32)).astype(out_ref.dtype)


def whole_kernel(peers, *refs):
    proj_ref, flat_ref, keep_ref, send_ref = refs[-4:]
    values_of(peers, refs, flat_ref)
    flat = flat_ref[...]
    columns = keep_ref.shape[2]
    span = math.lcm(2 * columns, 128)
    pairs = span // (2 * columns)
    for block in range(proj_ref.shape[1] // span):
        part = jnp.dot(
            flat,
            proj_ref[:, block * span : (block + 1) * span],
            preferred_element_type=jnp.float32,
        )
        for pair in range(pairs):
            share(part, pair, block * pairs + pair, keep_ref, send_ref)


def pair_kernel(keep_ref, got_ref, stay_ref, send_ref):
    side = lax.rem(lax.div(lax.axis_index("ctx"), 2), 2)
    for spot in range(stay_ref.shape[0]):
        mine = 2 * spot + side
        yours = 2 * spot + 1 - side
        stay_ref[spot] = keep_ref[mine] + got_ref[mine].astype(jnp.float32)
        send_ref[spot] = (keep_ref[yours] + got_ref[yours].astype(jnp.float32)).astype(jnp.bfloat16)


def quad_kernel(stay_ref, got_ref, own_ref, *out_refs):
    outer = lax.div(lax.axis_index("ctx"), 4)

    def both(spot):
        return stay_ref[spot] + got_ref[spot].astype(jnp.float32)

    for peer, out_ref in enumerate(out_refs, 1):
        out_ref[...] = both(lax.bitwise_xor(outer, peer)).astype(jnp.bfloat16)
    own_ref[...] = both(outer)


def call(kernel, outs, values, specs=None, out_specs=None, scratch=(), limit=24):
    return pl.pallas_call(
        kernel,
        out_shape=outs,
        in_specs=specs or [pl.BlockSpec() for _ in values],
        out_specs=out_specs or [pl.BlockSpec() for _ in outs],
        scratch_shapes=list(scratch),
        compiler_params=pltpu.CompilerParams(vmem_limit_bytes=limit << 20),
    )(*values)


def shaped(*shape, dtype=jnp.float32):
    return jax.ShapeDtypeStruct(shape, dtype)


def on_device(count, queries, cache, draft_latent, lengths, parents, value_up, out_proj):
    drafts, heads_here, width = queries.shape[1:]
    latent = value_up.shape[1]
    block_len = cache.shape[1]
    inner = 4
    outer = count // inner
    chips = count // 2
    columns = out_proj.shape[1] // count
    each = heads_here * drafts
    bf16 = jnp.bfloat16
    myself = lax.axis_index("ctx")

    def bias_of(*bits):
        spots = [
            lax.bitwise_xor(myself, bit) * block_len + jnp.arange(block_len, dtype=jnp.int32)
            for bit in bits
        ]
        live = jnp.concatenate(spots)[None, :] < lengths[0]
        return jnp.where(live, 0.0, neg_fill).astype(jnp.float32)

    def swap(value, bits):
        return lax.ppermute(value, "ctx", [(i, i ^ bits) for i in range(count)])

    def on_chip(value):
        return jnp.where(lengths[0] > -1, value, jnp.zeros_like(value))

    keys_own = jnp.transpose(cache[0])
    keys_across = swap(keys_own, 3)
    keys_core = swap(keys_own, 1)
    keys_far = swap(keys_across, 1)
    sent = {0: queries[0]}
    for peer in range(1, outer):
        sent[peer] = swap(queries[0], inner * peer + 1)
    rows = {
        peer: jnp.transpose(value, (1, 0, 2)).reshape(each, width) for peer, value in sent.items()
    }
    own_rows = rows[0]
    everyone = list(range(outer))

    def pick(table, peers):
        return [table[peer] for peer in peers]

    def state_of(blocks):
        return tuple(shaped(each, size) for size in (latent, 1, 1)) * blocks

    own_shape = state_of(1)
    proj_here = on_chip(out_proj)
    keys_here = on_chip(keys_own)
    state = {}

    def save(peers, values):
        for spot, peer in enumerate(peers):
            state[peer] = list(values[3 * spot : 3 * spot + 3])

    early = everyone[:2] + everyone[3:]
    for part in range(2):
        peers = [peer for peer in everyone if (peer in early) == (part == 0)]
        values = call(
            lambda *refs, size=len(peers): first_kernel(size, *refs),
            state_of(len(peers)),
            (bias_of(0, 1), *pick(rows, peers), keys_here, keys_core),
        )
        save(peers, values)
    values = call(
        lambda *refs: middle_kernel(outer, *refs),
        state_of(outer),
        (bias_of(3), *pick(rows, everyone), keys_across, *sum(pick(state, everyone), [])),
    )
    save(everyone, values)
    lanes = math.gcd(latent, 128)
    packed = shaped(each * latent // lanes + PACK_ROWS, lanes, dtype=bf16)
    got = []
    for near in (False, True):
        peers = everyone[: outer // 2] if near else everyone[outer // 2 :]
        values = call(
            lambda *refs, near=near: last_kernel(outer // 2, near, *refs),
            (own_shape if near else ()) + (packed,) * (len(peers) - near),
            (bias_of(2), *pick(rows, peers), keys_far, *sum(pick(state, peers), [])),
        )
        if near:
            whole, values, peers = values[:3], values[3:], peers[1:]
        got += [swap(value, inner * peer + 1) for peer, value in zip(peers, values)]
    proj_here = on_chip(out_proj)
    *whole, up_here = call(
        draft_kernel,
        own_shape + (shaped(*value_up.shape, dtype=bf16),),
        (own_rows, draft_latent[0], parents, value_up, *whole),
    )
    inputs = (*got, *whole, up_here, proj_here)
    flat_shape = shaped(drafts, heads_here * value_up.shape[2], dtype=bf16)

    def halves_of(chips):
        return shaped(chips, drafts, columns), shaped(chips, drafts, columns, dtype=bf16)

    cross = int(2 * columns % 128 == 0)
    if cross:
        flat, keep, send = call(
            lambda *refs: leaving_kernel(outer, *refs), (flat_shape, *halves_of(chips // 2)), inputs
        )
        got_leaving = swap(send, 1)
        stay, stay_send = call(staying_kernel, halves_of(chips // 2), (flat, proj_here))
        send = call(add_kernel, (halves_of(chips // 2)[1],), (keep, got_leaving))[0]
        got_staying = swap(stay_send, 1)
        stay = call(add_kernel, (halves_of(chips // 2)[0],), (stay, got_staying))[0]
    else:
        flat, keep, send = call(
            lambda *refs: whole_kernel(outer, *refs), (flat_shape, *halves_of(chips)), inputs
        )
        stay, send = call(pair_kernel, halves_of(chips // 2), (keep, swap(send, 1)))
    own, *parts = call(
        quad_kernel,
        (shaped(drafts, columns),)
        + tuple(shaped(drafts, columns, dtype=bf16) for _ in range(outer - 1)),
        (stay, swap(send, 2 + cross)),
    )
    result = own
    for peer in range(outer - 1, 0, -1):
        result = result + swap(parts[peer - 1], inner * peer + cross).astype(jnp.float32)
    return result.astype(bf16)


def solution(mesh):
    in_specs = (
        P("grp", None, "ctx", None),
        P("grp", "ctx", None),
        P("grp", None, None),
        P("grp"),
        P("grp", None),
        P("ctx", None, None),
        P("ctx", None),
    )
    count = mesh.shape["ctx"]

    def body(*args):
        return on_device(count, *args)

    return jax.shard_map(
        body, mesh=mesh, in_specs=in_specs, out_specs=P("grp", "ctx"), check_vma=False
    )
```

```python
import math

import jax
import jax.numpy as jnp
from jax import lax
from jax.experimental import pallas as pl
from jax.experimental.pallas import tpu as pltpu
from jax.sharding import PartitionSpec as P


yarn_factor = 1.0 + 0.1 * math.log(32.0)
score_scale = yarn_factor * yarn_factor / math.sqrt(192.0)
log2_scale = score_scale / math.log(2.0)
neg_fill = -1e30
low_top = -1e29
PACK_ROWS = 8


NT = (((1,), (1,)), ((), ()))


def weights_of(masked, top):
    weights = jnp.exp2(masked - top).astype(jnp.bfloat16)
    return weights, jnp.sum(weights.astype(jnp.float32), axis=1, keepdims=True)


def as_row(column):
    count = column.shape[0]
    eye = lax.broadcasted_iota(jnp.int32, (count, count), 0) == lax.broadcasted_iota(
        jnp.int32, (count, count), 1
    )
    return jnp.sum(jnp.where(eye, column, 0.0), axis=0, keepdims=True)


def as_column(row):
    count = row.shape[1]
    eye = lax.broadcasted_iota(jnp.int32, (count, count), 0) == lax.broadcasted_iota(
        jnp.int32, (count, count), 1
    )
    return jnp.sum(jnp.where(eye, row, 0.0), axis=1, keepdims=True)


def tree_bias(parents):
    drafts = parents.shape[1]
    order = lax.broadcasted_iota(jnp.int32, (drafts, drafts), 1)
    self_order = lax.broadcasted_iota(jnp.int32, (drafts, drafts), 0)
    parent = as_column(parents.astype(jnp.float32)).astype(jnp.int32)
    reach = jnp.where((parent == order) | (self_order == order), 1.0, 0.0)
    covered = 1
    while covered < drafts:
        step = reach.astype(jnp.bfloat16)
        grown = jnp.dot(step, step, preferred_element_type=jnp.float32)
        reach = jnp.where(grown > 0.5, 1.0, 0.0)
        covered *= 2
    return jnp.where(reach > 0.5, 0.0, neg_fill)


def merge(states):
    best = states[0][1]
    for state in states[1:]:
        best = jnp.maximum(best, state[1])
    numer = total = 0.0
    for part, top, count in states:
        factor = jnp.exp2(top - best)
        numer = numer + part * factor
        total = total + count * factor
    return numer, best, total


def draft_kernel(q_ref, keys_ref, parents_ref, up_from, *refs):
    own_refs, out_refs, up_ref = refs[:3], refs[3:6], refs[6]
    up_ref[...] = up_from[...]
    latent = own_refs[0].shape[1]
    keys = keys_ref[...]
    repeats = q_ref.shape[0] // keys.shape[0]
    bias = jnp.concatenate([tree_bias(parents_ref[...])] * repeats, axis=0)
    scores = lax.dot_general(q_ref[...], keys, NT, preferred_element_type=jnp.float32)
    masked = scores * log2_scale + bias
    top = jnp.max(masked, axis=1, keepdims=True)
    weights, total = weights_of(masked, top)
    numer = jnp.dot(weights, keys[:, :latent], preferred_element_type=jnp.float32)
    put(merge([(numer, top, total), tuple(ref[...] for ref in own_refs)]), out_refs)


def fold(rows, key_refs, bias_ref, carry, latent):
    blocks, tops = [], []
    at = 0
    for key_ref in key_refs:
        scores = jnp.dot(rows, key_ref[...], preferred_element_type=jnp.float32)
        masked = scores * log2_scale + bias_ref[:, at : at + key_ref.shape[1]]
        at += key_ref.shape[1]
        blocks.append(masked)
        tops.append(jnp.max(masked, axis=1, keepdims=True))
    top = carry[1] if carry is not None else jnp.full_like(tops[0], low_top)
    for other in tops:
        top = jnp.maximum(top, other)
    numer = total = None
    if carry is not None:
        factor = jnp.exp2(carry[1] - top)
        numer, total = carry[0] * factor, carry[2] * factor
    for key_ref, masked in zip(key_refs, blocks):
        weights, count = weights_of(masked, top)
        part = lax.dot_general(weights, key_ref[:latent, :], NT, preferred_element_type=jnp.float32)
        numer = part if numer is None else numer + part
        total = count if total is None else total + count
    return numer, top, total


def join_rows(q_refs):
    return jnp.concatenate([q[...] for q in q_refs], axis=0)


def put(state, refs):
    blocks = len(refs) // 3
    each = refs[0].shape[0]
    for block in range(blocks):
        for part in range(3):
            refs[3 * block + part][...] = state[part][block * each : (block + 1) * each]


def first_kernel(peers, bias_ref, *refs):
    q_refs, key_refs, out_refs = refs[:peers], refs[peers : -3 * peers], refs[-3 * peers :]
    put(fold(join_rows(q_refs), key_refs, bias_ref, None, out_refs[0].shape[1]), out_refs)


def carried(refs):
    return tuple(join_rows(refs[part::3]) for part in range(3))


def middle_kernel(peers, bias_ref, *refs):
    q_refs, (key_ref, *refs) = refs[:peers], refs[peers:]
    carry_refs, out_refs = refs[: 3 * peers], refs[3 * peers :]
    latent = out_refs[0].shape[1]
    put(fold(join_rows(q_refs), [key_ref], bias_ref, carried(carry_refs), latent), out_refs)


def pieces(row):
    high = row.astype(jnp.bfloat16).astype(jnp.float32)
    rest = row - high
    middle = rest.astype(jnp.bfloat16).astype(jnp.float32)
    return [high, middle, rest - middle]


def pack(numer, top, total, out_ref):
    each, latent = numer.shape
    lanes = out_ref.shape[1]
    for group in range(latent // lanes):
        strip = numer[:, group * lanes : (group + 1) * lanes]
        out_ref[group * each : (group + 1) * each, :] = strip.astype(jnp.bfloat16)
    lines = pieces(as_row(top)) + pieces(as_row(total))
    lines += [jnp.zeros_like(lines[0])] * (PACK_ROWS - len(lines))
    packed = jnp.concatenate(lines, axis=0)
    if lanes > each:
        packed = jnp.concatenate(
            [packed, jnp.zeros((PACK_ROWS, lanes - each), jnp.float32)], axis=1
        )
    out_ref[out_ref.shape[0] - PACK_ROWS :, :] = packed.astype(jnp.bfloat16)


def unpack(state_ref, each):
    bottom = state_ref.shape[0] - PACK_ROWS
    lines = state_ref[bottom:, :each].astype(jnp.float32)
    top = as_column(lines[0:1] + lines[1:2] + lines[2:3])
    total = as_column(lines[3:4] + lines[4:5] + lines[5:6])
    strips = [state_ref[at : at + each, :] for at in range(0, bottom, each)]
    return jnp.concatenate(strips, axis=1).astype(jnp.float32), top, total


def last_kernel(peers, plain, bias_ref, *refs):
    q_refs, (key_ref, *refs) = refs[:peers], refs[peers:]
    carry_refs, out_refs = refs[: 3 * peers], refs[3 * peers :]
    latent = carry_refs[0].shape[1]
    state = fold(join_rows(q_refs), [key_ref], bias_ref, carried(carry_refs), latent)
    each = q_refs[0].shape[0]
    if plain:
        put([value[:each] for value in state], out_refs[:3])
        out_refs = out_refs[3:]
    for peer, out_ref in enumerate(out_refs, 1 if plain else 0):
        pack(*(value[peer * each : (peer + 1) * each] for value in state), out_ref)


def values_of(peers, refs, flat_ref):
    state_refs, own_refs, up_ref = refs[: peers - 1], refs[peers - 1 : peers + 2], refs[peers + 2]
    each = own_refs[0].shape[0]
    heads, _, width = up_ref.shape
    drafts = each // heads
    states = [unpack(state, each) for state in state_refs]
    numer, _, total = merge([tuple(ref[...] for ref in own_refs)] + states)
    latent_out = (numer / total).astype(jnp.bfloat16)
    for head in range(heads):
        value = jnp.dot(
            latent_out[head * drafts : (head + 1) * drafts],
            up_ref[head],
            preferred_element_type=jnp.float32,
        )
        flat_ref[:, head * width : (head + 1) * width] = value.astype(jnp.bfloat16)


def share(part, pair, spot, keep_ref, send_ref, cross=0):
    columns = keep_ref.shape[2]
    first_core = lax.rem(lax.axis_index("ctx") + cross, 2) == 0
    halves = []
    for side in range(2):
        shift = (2 * pair + side) * columns
        moved = part if shift == 0 else pltpu.roll(part, part.shape[1] - shift, 1)
        halves.append(moved[:, :columns])
    keep_ref[spot] = jnp.where(first_core, halves[0], halves[1])
    send_ref[spot] = jnp.where(first_core, halves[1], halves[0]).astype(jnp.bfloat16)


def project_kernel(across, flat, proj_ref, keep_ref, send_ref):
    side = lax.rem(lax.div(lax.axis_index("ctx"), 2), 2)
    side = 1 - side if across else side
    outer = lax.div(lax.axis_index("ctx"), 4)
    span = 2 * keep_ref.shape[2]
    for spot in range(keep_ref.shape[0]):
        at = pl.multiple_of((2 * spot + side) * span, span)
        part = jnp.dot(flat, proj_ref[:, pl.ds(at, span)], preferred_element_type=jnp.float32)
        straight = outer == spot
        if across:
            straight |= outer == lax.bitwise_xor(spot, keep_ref.shape[0] - 1)
        share(part, 0, spot, keep_ref, send_ref, jnp.where(straight, 0, 1) + across)


def leaving_kernel(peers, *refs):
    proj_ref, flat_ref, keep_ref, send_ref = refs[-4:]
    values_of(peers, refs, flat_ref)
    project_kernel(1, flat_ref[...], proj_ref, keep_ref, send_ref)


def staying_kernel(flat_ref, proj_ref, keep_ref, send_ref):
    project_kernel(0, flat_ref[...], proj_ref, keep_ref, send_ref)


def add_kernel(keep_ref, got_ref, out_ref, direct_ref):
    outer = lax.div(lax.axis_index("ctx"), 4)
    for peer in range(keep_ref.shape[0]):
        spot = lax.bitwise_xor(outer, peer)
        value = keep_ref[spot] + got_ref[spot].astype(jnp.float32)
        if peer < out_ref.shape[0]:
            out_ref[peer] = value.astype(out_ref.dtype)
        else:
            direct_ref[...] = value.astype(direct_ref.dtype)


def depart_kernel(stay_ref, got_ref, own_ref, *out_refs):
    for peer, out_ref in enumerate((own_ref, *out_refs)):
        value = stay_ref[peer] + got_ref[peer].astype(jnp.float32)
        out_ref[...] = value.astype(out_ref.dtype)


def whole_kernel(peers, *refs):
    proj_ref, flat_ref, keep_ref, send_ref = refs[-4:]
    values_of(peers, refs, flat_ref)
    flat = flat_ref[...]
    columns = keep_ref.shape[2]
    span = math.lcm(2 * columns, 128)
    pairs = span // (2 * columns)
    for block in range(proj_ref.shape[1] // span):
        part = jnp.dot(
            flat,
            proj_ref[:, block * span : (block + 1) * span],
            preferred_element_type=jnp.float32,
        )
        for pair in range(pairs):
            share(part, pair, block * pairs + pair, keep_ref, send_ref)


def pair_kernel(keep_ref, got_ref, stay_ref, send_ref):
    side = lax.rem(lax.div(lax.axis_index("ctx"), 2), 2)
    for spot in range(stay_ref.shape[0]):
        mine = 2 * spot + side
        yours = 2 * spot + 1 - side
        stay_ref[spot] = keep_ref[mine] + got_ref[mine].astype(jnp.float32)
        send_ref[spot] = (keep_ref[yours] + got_ref[yours].astype(jnp.float32)).astype(jnp.bfloat16)


def quad_kernel(stay_ref, got_ref, own_ref, *out_refs):
    outer = lax.div(lax.axis_index("ctx"), 4)

    def both(spot):
        return stay_ref[spot] + got_ref[spot].astype(jnp.float32)

    for peer, out_ref in enumerate(out_refs, 1):
        out_ref[...] = both(lax.bitwise_xor(outer, peer)).astype(jnp.bfloat16)
    own_ref[...] = both(outer)


def call(kernel, outs, values, specs=None, out_specs=None, scratch=(), limit=24):
    return pl.pallas_call(
        kernel,
        out_shape=outs,
        in_specs=specs or [pl.BlockSpec() for _ in values],
        out_specs=out_specs or [pl.BlockSpec() for _ in outs],
        scratch_shapes=list(scratch),
        compiler_params=pltpu.CompilerParams(vmem_limit_bytes=limit << 20),
    )(*values)


def shaped(*shape, dtype=jnp.float32):
    return jax.ShapeDtypeStruct(shape, dtype)


def on_device(count, queries, cache, draft_latent, lengths, parents, value_up, out_proj):
    drafts, heads_here, width = queries.shape[1:]
    latent = value_up.shape[1]
    block_len = cache.shape[1]
    inner = 4
    outer = count // inner
    chips = count // 2
    columns = out_proj.shape[1] // count
    each = heads_here * drafts
    bf16 = jnp.bfloat16
    myself = lax.axis_index("ctx")

    def bias_of(*bits):
        spots = [
            lax.bitwise_xor(myself, bit) * block_len + jnp.arange(block_len, dtype=jnp.int32)
            for bit in bits
        ]
        live = jnp.concatenate(spots)[None, :] < lengths[0]
        return jnp.where(live, 0.0, neg_fill).astype(jnp.float32)

    def swap(value, bits):
        return lax.ppermute(value, "ctx", [(i, i ^ bits) for i in range(count)])

    def on_chip(value):
        return jnp.where(lengths[0] > -1, value, jnp.zeros_like(value))

    keys_own = jnp.transpose(cache[0])
    keys_across = swap(keys_own, 3)
    keys_core = swap(keys_own, 1)
    keys_far = swap(keys_across, 1)
    sent = {0: queries[0]}
    for peer in range(1, outer):
        sent[peer] = swap(queries[0], inner * peer + 1)
    rows = {
        peer: jnp.transpose(value, (1, 0, 2)).reshape(each, width) for peer, value in sent.items()
    }
    own_rows = rows[0]
    everyone = list(range(outer))

    def pick(table, peers):
        return [table[peer] for peer in peers]

    def state_of(blocks):
        return tuple(shaped(each, size) for size in (latent, 1, 1)) * blocks

    own_shape = state_of(1)
    proj_here = on_chip(out_proj)
    keys_here = on_chip(keys_own)
    state = {}

    def save(peers, values):
        for spot, peer in enumerate(peers):
            state[peer] = list(values[3 * spot : 3 * spot + 3])

    early = everyone[:2] + everyone[3:]
    for part in range(2):
        peers = [peer for peer in everyone if (peer in early) == (part == 0)]
        values = call(
            lambda *refs, size=len(peers): first_kernel(size, *refs),
            state_of(len(peers)),
            (bias_of(0, 1), *pick(rows, peers), keys_here, keys_core),
        )
        save(peers, values)
    values = call(
        lambda *refs: middle_kernel(outer, *refs),
        state_of(outer),
        (bias_of(3), *pick(rows, everyone), keys_across, *sum(pick(state, everyone), [])),
    )
    save(everyone, values)
    lanes = math.gcd(latent, 128)
    packed = shaped(each * latent // lanes + PACK_ROWS, lanes, dtype=bf16)
    got = []
    for near in (False, True):
        peers = everyone[: outer // 2] if near else everyone[outer // 2 :]
        values = call(
            lambda *refs, near=near: last_kernel(outer // 2, near, *refs),
            (own_shape if near else ()) + (packed,) * (len(peers) - near),
            (bias_of(2), *pick(rows, peers), keys_far, *sum(pick(state, peers), [])),
        )
        if near:
            whole, values, peers = values[:3], values[3:], peers[1:]
        got += [swap(value, inner * peer + 1) for peer, value in zip(peers, values)]
    proj_here = on_chip(out_proj)
    *whole, up_here = call(
        draft_kernel,
        own_shape + (shaped(*value_up.shape, dtype=bf16),),
        (own_rows, draft_latent[0], parents, value_up, *whole),
    )
    inputs = (*got, *whole, up_here, proj_here)
    flat_shape = shaped(drafts, heads_here * value_up.shape[2], dtype=bf16)

    def halves_of(chips):
        return shaped(chips, drafts, columns), shaped(chips, drafts, columns, dtype=bf16)

    cross = int(2 * columns % 128 == 0)
    if cross:
        flat, keep, send = call(
            lambda *refs: leaving_kernel(outer, *refs), (flat_shape, *halves_of(chips // 2)), inputs
        )
        got_leaving = swap(send, 1)
        stay, stay_send = call(staying_kernel, halves_of(chips // 2), (flat, proj_here))
        thin = shaped(drafts, columns, dtype=bf16)
        wide, narrow = halves_of(outer - 1)
        leave, direct_across = call(add_kernel, (narrow, thin), (keep, got_leaving))
        got_staying = swap(stay_send, 1)
        stay, direct = call(add_kernel, (wide, thin), (stay, got_staying))
        last = inner * (outer - 1)
        came = [swap(direct, last + 1), swap(direct_across, last + 3)]
        own, *parts = call(
            depart_kernel,
            (shaped(drafts, columns),) + (thin,) * (outer - 2),
            (stay, swap(leave, 3)),
        )
    else:
        flat, keep, send = call(
            lambda *refs: whole_kernel(outer, *refs), (flat_shape, *halves_of(chips)), inputs
        )
        stay, send = call(pair_kernel, halves_of(chips // 2), (keep, swap(send, 1)))
        own, *parts = call(
            quad_kernel,
            (shaped(drafts, columns),)
            + tuple(shaped(drafts, columns, dtype=bf16) for _ in range(outer - 1)),
            (stay, swap(send, 2)),
        )
        came = []
    for peer in range(len(parts), 0, -1):
        came.append(swap(parts[peer - 1], inner * peer + cross))
    result = own
    for value in came:
        result = result + value.astype(jnp.float32)
    return result.astype(bf16)


def solution(mesh):
    in_specs = (
        P("grp", None, "ctx", None),
        P("grp", "ctx", None),
        P("grp", None, None),
        P("grp"),
        P("grp", None),
        P("ctx", None, None),
        P("ctx", None),
    )
    count = mesh.shape["ctx"]

    def body(*args):
        return on_device(count, *args)

    return jax.shard_map(
        body, mesh=mesh, in_specs=in_specs, out_specs=P("grp", "ctx"), check_vma=False
    )
```

```python
import math

import jax
import jax.numpy as jnp
from jax import lax
from jax.experimental import pallas as pl
from jax.experimental.pallas import tpu as pltpu
from jax.sharding import PartitionSpec as P


yarn_factor = 1.0 + 0.1 * math.log(32.0)
score_scale = yarn_factor * yarn_factor / math.sqrt(192.0)
log2_scale = score_scale / math.log(2.0)
neg_fill = -1e30
low_top = -1e29
PACK_ROWS = 8


NT = (((1,), (1,)), ((), ()))


def weights_of(masked, top):
    weights = jnp.exp2(masked - top).astype(jnp.bfloat16)
    return weights, jnp.sum(weights.astype(jnp.float32), axis=1, keepdims=True)


def as_row(column):
    count = column.shape[0]
    eye = lax.broadcasted_iota(jnp.int32, (count, count), 0) == lax.broadcasted_iota(
        jnp.int32, (count, count), 1
    )
    return jnp.sum(jnp.where(eye, column, 0.0), axis=0, keepdims=True)


def as_column(row):
    count = row.shape[1]
    eye = lax.broadcasted_iota(jnp.int32, (count, count), 0) == lax.broadcasted_iota(
        jnp.int32, (count, count), 1
    )
    return jnp.sum(jnp.where(eye, row, 0.0), axis=1, keepdims=True)


def tree_bias(parents):
    drafts = parents.shape[1]
    order = lax.broadcasted_iota(jnp.int32, (drafts, drafts), 1)
    self_order = lax.broadcasted_iota(jnp.int32, (drafts, drafts), 0)
    parent = as_column(parents.astype(jnp.float32)).astype(jnp.int32)
    reach = jnp.where((parent == order) | (self_order == order), 1.0, 0.0)
    covered = 1
    while covered < drafts:
        step = reach.astype(jnp.bfloat16)
        grown = jnp.dot(step, step, preferred_element_type=jnp.float32)
        reach = jnp.where(grown > 0.5, 1.0, 0.0)
        covered *= 2
    return jnp.where(reach > 0.5, 0.0, neg_fill)


def merge(states):
    best = states[0][1]
    for state in states[1:]:
        best = jnp.maximum(best, state[1])
    numer = total = 0.0
    for part, top, count in states:
        factor = jnp.exp2(top - best)
        numer = numer + part * factor
        total = total + count * factor
    return numer, best, total


def draft_kernel(q_ref, keys_ref, parents_ref, up_from, *refs):
    own_refs, out_refs, up_ref = refs[:3], refs[3:6], refs[6]
    up_ref[...] = up_from[...]
    latent = own_refs[0].shape[1]
    keys = keys_ref[...]
    repeats = q_ref.shape[0] // keys.shape[0]
    bias = jnp.concatenate([tree_bias(parents_ref[...])] * repeats, axis=0)
    scores = lax.dot_general(q_ref[...], keys, NT, preferred_element_type=jnp.float32)
    masked = scores * log2_scale + bias
    top = jnp.max(masked, axis=1, keepdims=True)
    weights, total = weights_of(masked, top)
    numer = jnp.dot(weights, keys[:, :latent], preferred_element_type=jnp.float32)
    put(merge([(numer, top, total), tuple(ref[...] for ref in own_refs)]), out_refs)


def fold(rows, key_refs, bias_ref, carry, latent):
    blocks, tops = [], []
    at = 0
    for key_ref in key_refs:
        scores = jnp.dot(rows, key_ref[...], preferred_element_type=jnp.float32)
        masked = scores * log2_scale + bias_ref[:, at : at + key_ref.shape[1]]
        at += key_ref.shape[1]
        blocks.append(masked)
        tops.append(jnp.max(masked, axis=1, keepdims=True))
    top = carry[1] if carry is not None else jnp.full_like(tops[0], low_top)
    for other in tops:
        top = jnp.maximum(top, other)
    numer = total = None
    if carry is not None:
        factor = jnp.exp2(carry[1] - top)
        numer, total = carry[0] * factor, carry[2] * factor
    for key_ref, masked in zip(key_refs, blocks):
        weights, count = weights_of(masked, top)
        part = lax.dot_general(weights, key_ref[:latent, :], NT, preferred_element_type=jnp.float32)
        numer = part if numer is None else numer + part
        total = count if total is None else total + count
    return numer, top, total


def join_rows(q_refs):
    return jnp.concatenate([q[...] for q in q_refs], axis=0)


def put(state, refs):
    blocks = len(refs) // 3
    each = refs[0].shape[0]
    for block in range(blocks):
        for part in range(3):
            refs[3 * block + part][...] = state[part][block * each : (block + 1) * each]


def first_kernel(peers, bias_ref, *refs):
    q_refs, key_refs, out_refs = refs[:peers], refs[peers : -3 * peers], refs[-3 * peers :]
    put(fold(join_rows(q_refs), key_refs, bias_ref, None, out_refs[0].shape[1]), out_refs)


def carried(refs):
    return tuple(join_rows(refs[part::3]) for part in range(3))


def middle_kernel(peers, bias_ref, *refs):
    q_refs, (key_ref, *refs) = refs[:peers], refs[peers:]
    carry_refs, out_refs = refs[: 3 * peers], refs[3 * peers :]
    latent = out_refs[0].shape[1]
    put(fold(join_rows(q_refs), [key_ref], bias_ref, carried(carry_refs), latent), out_refs)


def pieces(row):
    high = row.astype(jnp.bfloat16).astype(jnp.float32)
    rest = row - high
    middle = rest.astype(jnp.bfloat16).astype(jnp.float32)
    return [high, middle, rest - middle]


def pack(numer, top, total, out_ref):
    each, latent = numer.shape
    lanes = out_ref.shape[1]
    for group in range(latent // lanes):
        strip = numer[:, group * lanes : (group + 1) * lanes]
        out_ref[group * each : (group + 1) * each, :] = strip.astype(jnp.bfloat16)
    lines = pieces(as_row(top)) + pieces(as_row(total))
    lines += [jnp.zeros_like(lines[0])] * (PACK_ROWS - len(lines))
    packed = jnp.concatenate(lines, axis=0)
    if lanes > each:
        packed = jnp.concatenate(
            [packed, jnp.zeros((PACK_ROWS, lanes - each), jnp.float32)], axis=1
        )
    out_ref[out_ref.shape[0] - PACK_ROWS :, :] = packed.astype(jnp.bfloat16)


def unpack(state_ref, each):
    bottom = state_ref.shape[0] - PACK_ROWS
    lines = state_ref[bottom:, :each].astype(jnp.float32)
    top = as_column(lines[0:1] + lines[1:2] + lines[2:3])
    total = as_column(lines[3:4] + lines[4:5] + lines[5:6])
    strips = [state_ref[at : at + each, :] for at in range(0, bottom, each)]
    return jnp.concatenate(strips, axis=1).astype(jnp.float32), top, total


def last_kernel(peers, plain, bias_ref, *refs):
    q_refs, (key_ref, *refs) = refs[:peers], refs[peers:]
    carry_refs, out_refs = refs[: 3 * peers], refs[3 * peers :]
    latent = carry_refs[0].shape[1]
    state = fold(join_rows(q_refs), [key_ref], bias_ref, carried(carry_refs), latent)
    each = q_refs[0].shape[0]
    if plain:
        put([value[:each] for value in state], out_refs[:3])
        out_refs = out_refs[3:]
    for peer, out_ref in enumerate(out_refs, 1 if plain else 0):
        pack(*(value[peer * each : (peer + 1) * each] for value in state), out_ref)


def values_of(peers, refs, flat_ref):
    state_refs, own_refs, up_ref = refs[: peers - 1], refs[peers - 1 : peers + 2], refs[peers + 2]
    each = own_refs[0].shape[0]
    heads, _, width = up_ref.shape
    drafts = each // heads
    states = [unpack(state, each) for state in state_refs]
    numer, _, total = merge([tuple(ref[...] for ref in own_refs)] + states)
    latent_out = (numer / total).astype(jnp.bfloat16)
    for head in range(heads):
        value = jnp.dot(
            latent_out[head * drafts : (head + 1) * drafts],
            up_ref[head],
            preferred_element_type=jnp.float32,
        )
        flat_ref[:, head * width : (head + 1) * width] = value.astype(jnp.bfloat16)


def share(part, pair, spot, keep_ref, send_ref, cross=0):
    columns = keep_ref.shape[2]
    first_core = lax.rem(lax.axis_index("ctx") + cross, 2) == 0
    halves = []
    for side in range(2):
        shift = (2 * pair + side) * columns
        moved = part if shift == 0 else pltpu.roll(part, part.shape[1] - shift, 1)
        halves.append(moved[:, :columns])
    keep_ref[spot] = jnp.where(first_core, halves[0], halves[1])
    send_ref[spot] = jnp.where(first_core, halves[1], halves[0]).astype(jnp.bfloat16)


def direct_peer():
    return 1


def sum_order(outer):
    direct = direct_peer()
    return [peer for peer in range(outer) if peer != direct] + [direct]


def project_kernel(across, flat, proj_ref, keep_ref, send_ref):
    side = lax.rem(lax.div(lax.axis_index("ctx"), 2), 2)
    side = 1 - side if across else side
    outer = lax.div(lax.axis_index("ctx"), 4)
    span = 2 * keep_ref.shape[2]
    for spot in range(keep_ref.shape[0]):
        at = pl.multiple_of((2 * spot + side) * span, span)
        part = jnp.dot(flat, proj_ref[:, pl.ds(at, span)], preferred_element_type=jnp.float32)
        straight = outer == spot
        if across:
            straight |= outer == lax.bitwise_xor(spot, direct_peer())
        share(part, 0, spot, keep_ref, send_ref, jnp.where(straight, 0, 1) + across)


def leaving_kernel(peers, *refs):
    proj_ref, flat_ref, keep_ref, send_ref = refs[-4:]
    values_of(peers, refs, flat_ref)
    project_kernel(1, flat_ref[...], proj_ref, keep_ref, send_ref)


def staying_kernel(flat_ref, proj_ref, keep_ref, send_ref):
    project_kernel(0, flat_ref[...], proj_ref, keep_ref, send_ref)


def add_kernel(keep_ref, got_ref, out_ref, direct_ref):
    outer = lax.div(lax.axis_index("ctx"), 4)
    for place, peer in enumerate(sum_order(keep_ref.shape[0])):
        spot = lax.bitwise_xor(outer, peer)
        value = keep_ref[spot] + got_ref[spot].astype(jnp.float32)
        if place < out_ref.shape[0]:
            out_ref[place] = value.astype(out_ref.dtype)
        else:
            direct_ref[...] = value.astype(direct_ref.dtype)


def depart_kernel(stay_ref, got_ref, own_ref, *out_refs):
    for peer, out_ref in enumerate((own_ref, *out_refs)):
        value = stay_ref[peer] + got_ref[peer].astype(jnp.float32)
        out_ref[...] = value.astype(out_ref.dtype)


def whole_kernel(peers, *refs):
    proj_ref, flat_ref, keep_ref, send_ref = refs[-4:]
    values_of(peers, refs, flat_ref)
    flat = flat_ref[...]
    columns = keep_ref.shape[2]
    span = math.lcm(2 * columns, 128)
    pairs = span // (2 * columns)
    for block in range(proj_ref.shape[1] // span):
        part = jnp.dot(
            flat,
            proj_ref[:, block * span : (block + 1) * span],
            preferred_element_type=jnp.float32,
        )
        for pair in range(pairs):
            share(part, pair, block * pairs + pair, keep_ref, send_ref)


def pair_kernel(keep_ref, got_ref, stay_ref, send_ref):
    side = lax.rem(lax.div(lax.axis_index("ctx"), 2), 2)
    for spot in range(stay_ref.shape[0]):
        mine = 2 * spot + side
        yours = 2 * spot + 1 - side
        stay_ref[spot] = keep_ref[mine] + got_ref[mine].astype(jnp.float32)
        send_ref[spot] = (keep_ref[yours] + got_ref[yours].astype(jnp.float32)).astype(jnp.bfloat16)


def quad_kernel(stay_ref, got_ref, own_ref, *out_refs):
    outer = lax.div(lax.axis_index("ctx"), 4)

    def both(spot):
        return stay_ref[spot] + got_ref[spot].astype(jnp.float32)

    for peer, out_ref in enumerate(out_refs, 1):
        out_ref[...] = both(lax.bitwise_xor(outer, peer)).astype(jnp.bfloat16)
    own_ref[...] = both(outer)


def call(kernel, outs, values, specs=None, out_specs=None, scratch=(), limit=24):
    return pl.pallas_call(
        kernel,
        out_shape=outs,
        in_specs=specs or [pl.BlockSpec() for _ in values],
        out_specs=out_specs or [pl.BlockSpec() for _ in outs],
        scratch_shapes=list(scratch),
        compiler_params=pltpu.CompilerParams(vmem_limit_bytes=limit << 20),
    )(*values)


def shaped(*shape, dtype=jnp.float32):
    return jax.ShapeDtypeStruct(shape, dtype)


def on_device(count, queries, cache, draft_latent, lengths, parents, value_up, out_proj):
    drafts, heads_here, width = queries.shape[1:]
    latent = value_up.shape[1]
    block_len = cache.shape[1]
    inner = 4
    outer = count // inner
    chips = count // 2
    columns = out_proj.shape[1] // count
    each = heads_here * drafts
    bf16 = jnp.bfloat16
    myself = lax.axis_index("ctx")

    def bias_of(*bits):
        spots = [
            lax.bitwise_xor(myself, bit) * block_len + jnp.arange(block_len, dtype=jnp.int32)
            for bit in bits
        ]
        live = jnp.concatenate(spots)[None, :] < lengths[0]
        return jnp.where(live, 0.0, neg_fill).astype(jnp.float32)

    def swap(value, bits):
        return lax.ppermute(value, "ctx", [(i, i ^ bits) for i in range(count)])

    def on_chip(value):
        return jnp.where(lengths[0] > -1, value, jnp.zeros_like(value))

    keys_own = jnp.transpose(cache[0])
    keys_across = swap(keys_own, 3)
    keys_core = swap(keys_own, 1)
    keys_far = swap(keys_across, 1)
    sent = {0: queries[0]}
    for peer in range(1, outer):
        sent[peer] = swap(queries[0], inner * peer + 1)
    rows = {
        peer: jnp.transpose(value, (1, 0, 2)).reshape(each, width) for peer, value in sent.items()
    }
    own_rows = rows[0]
    everyone = list(range(outer))

    def pick(table, peers):
        return [table[peer] for peer in peers]

    def state_of(blocks):
        return tuple(shaped(each, size) for size in (latent, 1, 1)) * blocks

    own_shape = state_of(1)
    proj_here = on_chip(out_proj)
    keys_here = on_chip(keys_own)
    state = {}

    def save(peers, values):
        for spot, peer in enumerate(peers):
            state[peer] = list(values[3 * spot : 3 * spot + 3])

    early = everyone[:2] + everyone[3:]
    for part in range(2):
        peers = [peer for peer in everyone if (peer in early) == (part == 0)]
        values = call(
            lambda *refs, size=len(peers): first_kernel(size, *refs),
            state_of(len(peers)),
            (bias_of(0, 1), *pick(rows, peers), keys_here, keys_core),
        )
        save(peers, values)
    values = call(
        lambda *refs: middle_kernel(outer, *refs),
        state_of(outer),
        (bias_of(3), *pick(rows, everyone), keys_across, *sum(pick(state, everyone), [])),
    )
    save(everyone, values)
    lanes = math.gcd(latent, 128)
    packed = shaped(each * latent // lanes + PACK_ROWS, lanes, dtype=bf16)
    got = []
    for near in (False, True):
        peers = everyone[: outer // 2] if near else everyone[outer // 2 :]
        values = call(
            lambda *refs, near=near: last_kernel(outer // 2, near, *refs),
            (own_shape if near else ()) + (packed,) * (len(peers) - near),
            (bias_of(2), *pick(rows, peers), keys_far, *sum(pick(state, peers), [])),
        )
        if near:
            whole, values, peers = values[:3], values[3:], peers[1:]
        got += [swap(value, inner * peer + 1) for peer, value in zip(peers, values)]
    proj_here = on_chip(out_proj)
    *whole, up_here = call(
        draft_kernel,
        own_shape + (shaped(*value_up.shape, dtype=bf16),),
        (own_rows, draft_latent[0], parents, value_up, *whole),
    )
    inputs = (*got, *whole, up_here, proj_here)
    flat_shape = shaped(drafts, heads_here * value_up.shape[2], dtype=bf16)

    def halves_of(chips):
        return shaped(chips, drafts, columns), shaped(chips, drafts, columns, dtype=bf16)

    cross = int(2 * columns % 128 == 0)
    if cross:
        flat, keep, send = call(
            lambda *refs: leaving_kernel(outer, *refs), (flat_shape, *halves_of(chips // 2)), inputs
        )
        got_leaving = swap(send, 1)
        stay, stay_send = call(staying_kernel, halves_of(chips // 2), (flat, proj_here))
        thin = shaped(drafts, columns, dtype=bf16)
        wide, narrow = halves_of(outer - 1)
        leave, direct_across = call(add_kernel, (narrow, thin), (keep, got_leaving))
        got_staying = swap(stay_send, 1)
        stay, direct = call(add_kernel, (wide, thin), (stay, got_staying))
        last = inner * direct_peer()
        later = sum_order(outer)[1:-1]
        came = [swap(direct, last + 1), swap(direct_across, last + 3)]
        own, *parts = call(
            depart_kernel,
            (shaped(drafts, columns),) + (thin,) * (outer - 2),
            (stay, swap(leave, 3)),
        )
    else:
        flat, keep, send = call(
            lambda *refs: whole_kernel(outer, *refs), (flat_shape, *halves_of(chips)), inputs
        )
        stay, send = call(pair_kernel, halves_of(chips // 2), (keep, swap(send, 1)))
        own, *parts = call(
            quad_kernel,
            (shaped(drafts, columns),)
            + tuple(shaped(drafts, columns, dtype=bf16) for _ in range(outer - 1)),
            (stay, swap(send, 2)),
        )
        came = []
        later = list(range(1, outer))
    for peer, value in zip(later, parts):
        came.append(swap(value, inner * peer + cross))
    result = own
    for value in came:
        result = result + value.astype(jnp.float32)
    return result.astype(bf16)


def solution(mesh):
    in_specs = (
        P("grp", None, "ctx", None),
        P("grp", "ctx", None),
        P("grp", None, None),
        P("grp"),
        P("grp", None),
        P("ctx", None, None),
        P("ctx", None),
    )
    count = mesh.shape["ctx"]

    def body(*args):
        return on_device(count, *args)

    return jax.shard_map(
        body, mesh=mesh, in_specs=in_specs, out_specs=P("grp", "ctx"), check_vma=False
    )
```
